32 devices in a mesh: strip: 8 (over z, x), seq: 4 (over y, core).
Axes of the slice: x: 2, y: 2, z: 4, core: 2. Of those that a mesh axis runs over, the one named last changes fastest.
Arguments:
- patches: bfloat16 [32, 536, 768], P('strip', 'seq'), may hold values from -6 to 6
- lengths: int32 [32], P('strip'), may hold values from 1 to 536, as said below
- script: int32 [32], P('strip'), may hold values from 0 to 3, as said below
- script_table: bfloat16 [4, 768], replicated, may hold values from -3 to 3
- gain_one: float32 [768], replicated, may hold values from 0.25 to 1.75
- bias_one: float32 [768], replicated, may hold values from -2 to 2
- qkv_weight: bfloat16 [768, 2304], replicated, may hold values from -0.3125 to 0.3125
- query_bias: float32 [768], replicated, may hold values from -3 to 3
- value_bias: float32 [768], replicated, may hold values from -3 to 3
- out_weight: bfloat16 [768, 768], replicated, may hold values from -0.875 to 0.875
- out_bias: float32 [768], replicated, may hold values from -3 to 3
- gain_two: float32 [768], replicated, may hold values from 0.25 to 1.75
- bias_two: float32 [768], replicated, may hold values from -2 to 2
- up_weight: bfloat16 [768, 3072], replicated, may hold values from -0.21875 to 0.21875
- up_bias: float32 [3072], replicated, may hold values from -3 to 3
- down_weight: bfloat16 [3072, 768], replicated, may hold values from -0.109375 to 0.109375
- down_bias: float32 [768], replicated, may hold values from -3 to 3
- cotangent: bfloat16 [32, 536, 768], P('strip', 'seq'), may hold values from -6 to 6
Outputs:
- layer_out: bfloat16 [32, 536, 768], P('strip', 'seq')
- grad_patches: bfloat16 [32, 536, 768], P('strip', 'seq')
- grad_table: float32 [768, 4], P(('strip', 'seq'))
- grad_gain_one: float32 [768], P(('strip', 'seq'))
- grad_bias_one: float32 [768], P(('strip', 'seq'))
- grad_qkv: float32 [768, 2304], P(('strip', 'seq'))
- grad_query_bias: float32 [768], P(('strip', 'seq'))
- grad_value_bias: float32 [768], P(('strip', 'seq'))
- grad_out_weight: float32 [768, 768], P(('strip', 'seq'))
- grad_out_bias: float32 [768], P(('strip', 'seq'))
- grad_gain_two: float32 [768], P(('strip', 'seq'))
- grad_bias_two: float32 [768], P(('strip', 'seq'))
- grad_up_weight: float32 [768, 3072], P(('strip', 'seq'))
- grad_up_bias: float32 [3072], P(('strip', 'seq'))
- grad_down_weight: float32 [3072, 768], P(('strip', 'seq'))
- grad_down_bias: float32 [768], P(('strip', 'seq'))
The draws below stay inside these ranges and needn't reach their ends.
Inputs may be any that keep to these rules, and one draw needn't show every extreme that they name: The first lengths[s] patch slots of strip s are filled; some strip has all 536 filled. `script`: script ids never fall from one strip to the next.
All inputs are finite; a program needn't handle non-finite values.
Results may differ from the reference program's by a relative error of at most 0.013.
The reference program's roundings to bfloat16 on the way count: a program that leaves them out, or rounds other values in their place, can miss the bound.
Values may be sent and summed in bfloat16 or wider, within the bound.
A program may use at most 192 MiB of HBM per device.

```python
import jax
import jax.numpy as jnp
from jax import lax

D = 768
HEADS = 12
HD = 64
FF = 3072
L = 536
GROUPS = 4
STRIP_DEV = 4
STRIPS = 32


def script_order(key):
    script_ids = jax.random.randint(jax.random.fold_in(key, 7), (STRIPS,), 0, GROUPS)
    script_ids = script_ids.at[0].set(0)
    return jnp.sort(script_ids)


def draw_script(key, part):
    return script_order(key).astype(jnp.int32)


def draw_lengths(key, part):
    ordered = script_order(key)
    lowest = jnp.where(ordered == 0, L - L // 10, jnp.where(ordered == 1, 1, jnp.where(ordered == 2, L // 4, L // 3)))
    highest = jnp.where(ordered == 0, L, jnp.where(ordered == 1, L // 3, jnp.where(ordered == 2, L // 2, 2 * L // 3)))
    spread = jax.random.randint(jax.random.fold_in(key, 11), (STRIPS,), 0, 1 << 20)
    filled = lowest + spread % (highest - lowest + 1)
    return filled.at[0].set(L).astype(jnp.int32)


def spiked(entries, own_key, source, target, parts, factor):
    owner, partner = [(jnp.arange(entries.shape[dim]) // (entries.shape[dim] // parts)).reshape([-1 if axis == dim else 1 for axis in range(entries.ndim)]) for dim in (source, target)]
    chosen = jax.random.permutation(own_key, parts)[partner]
    strong = (owner == chosen) | (owner == (partner + parts // 2) % parts)
    return jnp.where(strong, factor * entries, entries)


def block_levels(key, dims, shards, low, largest):
    gain, own = 1.0, jax.random.fold_in(key, 6)
    for dim, parts in shards:
        steps = jnp.exp(jax.random.uniform(jax.random.fold_in(own, dim), (parts,), jnp.float32, low / len(shards), largest / len(shards)))
        gain = gain * jnp.repeat(steps, dims[dim] // parts).reshape([-1 if axis == dim else 1 for axis in range(len(dims))])
    return gain


def gaussian(key, dims, scale, limit, shards=(), dtype=jnp.bfloat16):
    entries = jax.random.normal(key, dims, jnp.float32) * scale
    if len(shards) > 0:
        entries = block_levels(key, dims, shards, -0.22, 0.18) * entries
    return jnp.clip(entries, min=-limit, max=limit).astype(dtype)


def gaussian_with(stream_key, extent, scale, most, pieces, heavy, dtype=jnp.bfloat16):
    drawn = scale * jax.random.normal(stream_key, extent, jnp.float32)
    if pieces:
        drawn = drawn * block_levels(stream_key, extent, pieces, -0.22, 0.18)
    return jnp.clip(spiked(drawn, jax.random.fold_in(stream_key, 3), *heavy), -most, most).astype(dtype)


def setup_inputs(seed: int = 0) -> dict:
    keys = jax.random.split(jax.random.key(seed), 19)
    patches = gaussian(keys[0], (STRIPS, L, D), 1.0, 6.0, ((0, 8), (1, 4)))
    lengths = draw_lengths(jax.random.fold_in(keys[18], 71), 0)
    script = draw_script(jax.random.fold_in(keys[18], 71), 0)
    script_table = gaussian(keys[3], (GROUPS, D), 0.5, 3.0)
    gain_one = jnp.clip(1.0 + 0.15 * jax.random.normal(keys[4], (D,), jnp.float32), 0.25, 1.75)
    bias_one = gaussian(keys[5], (D,), 0.3, 2.0, (), jnp.float32)
    qkv_weight = gaussian(keys[6], (D, 3 * D), (D // 2) ** -0.5, 0.3125)
    query_bias = gaussian(keys[7], (D,), 0.5, 3.0, (), jnp.float32)
    value_bias = gaussian(keys[8], (D,), 0.5, 3.0, (), jnp.float32)
    out_weight = gaussian(keys[9], (D, D), (D // 16) ** -0.5, 0.875)
    out_bias = gaussian(keys[10], (D,), 0.5, 3.0, (), jnp.float32)
    gain_two = jnp.clip(1.0 + 0.15 * jax.random.normal(keys[11], (D,), jnp.float32), 0.25, 1.75)
    bias_two = gaussian(keys[12], (D,), 0.3, 2.0, (), jnp.float32)
    up_weight = gaussian(keys[13], (D, FF), D ** -0.5, 0.21875)
    up_bias = gaussian(keys[14], (FF,), 0.5, 3.0, (), jnp.float32)
    down_weight = gaussian(keys[15], (FF, D), FF ** -0.5, 0.109375)
    down_bias = gaussian(keys[16], (D,), 0.5, 3.0, (), jnp.float32)
    cotangent = gaussian_with(keys[17], (STRIPS, L, D), 1.0, 6.0, ((0, 8), (1, 4)), (0, 2, 8, 2.0))
    return {"patches": patches, "lengths": lengths, "script": script, "script_table": script_table, "gain_one": gain_one, "bias_one": bias_one, "qkv_weight": qkv_weight, "query_bias": query_bias, "value_bias": value_bias, "out_weight": out_weight, "out_bias": out_bias, "gain_two": gain_two, "bias_two": bias_two, "up_weight": up_weight, "up_bias": up_bias, "down_weight": down_weight, "down_bias": down_bias, "cotangent": cotangent}


@jax.custom_vjp
def low(v):
    return lax.optimization_barrier(v.astype(jnp.bfloat16)).astype(jnp.float32)

@jax.custom_vjp
def low_back(v):
    return v

def low_keep(v):
    return (low(v), None)

def low_pass(kept, grad):
    return (grad,)

def back_keep(v):
    return (v, None)

def back_low(kept, grad):
    return (low(grad),)
low.defvjp(low_keep, low_pass)
low_back.defvjp(back_keep, back_low)

def normalize(hidden):
    centred = hidden - lax.optimization_barrier(jnp.mean(hidden, axis=-1, keepdims=True))
    return centred * lax.rsqrt(lax.optimization_barrier(jnp.mean(centred * centred, axis=-1, keepdims=True)) + 1e-12)

def layer(patches, table, gain_one, bias_one, qkv_weight, query_bias, value_bias, out_weight, out_bias, gain_two, bias_two, up_weight, up_bias, down_weight, down_bias, selector, visible):
    highest = lax.Precision.HIGHEST
    batch = patches.shape[0]
    hidden = patches + jnp.einsum('bg,gd->bd', selector, table, precision=highest)[:, None, :]
    normed = low(normalize(hidden) * gain_one + bias_one)
    joint_bias = jnp.concatenate([query_bias, jnp.zeros_like(query_bias), value_bias])
    projected = jnp.einsum('bld,de->ble', normed, qkv_weight, precision=highest) + joint_bias
    projected = low_back(low(projected)).reshape(batch, L, 3, HEADS, HD)
    logits = jnp.einsum('bqhd,bkhd->bhqk', projected[:, :, 0], projected[:, :, 1], precision=highest) * HD ** (-0.5)
    logits = jnp.where(visible[:, None, None, :], low_back(logits), -1000000000.0)
    probs = low(jax.nn.softmax(logits, axis=-1))
    mixed = jnp.einsum('bhqk,bkhd->bqhd', probs, projected[:, :, 2], precision=highest)
    mixed = low_back(low(mixed)).reshape(batch, L, D)
    hidden = hidden + low_back(jnp.einsum('bld,de->ble', mixed, out_weight, precision=highest) + out_bias)
    normed = low(normalize(hidden) * gain_two + bias_two)
    upper = low_back(jnp.einsum('bld,df->blf', normed, up_weight, precision=highest) + up_bias)
    active = low(jax.nn.gelu(upper, approximate=False))
    return hidden + low_back(jnp.einsum('blf,fd->bld', active, down_weight, precision=highest) + down_bias)

def reference(patches, lengths, script, script_table, gain_one, bias_one, qkv_weight, query_bias, value_bias, out_weight, out_bias, gain_two, bias_two, up_weight, up_bias, down_weight, down_bias, cotangent):
    params = tuple((w.astype(jnp.float32) for w in (script_table, gain_one, bias_one, qkv_weight, query_bias, value_bias, out_weight, out_bias, gain_two, bias_two, up_weight, up_bias, down_weight, down_bias)))
    blocks_count = STRIPS // STRIP_DEV
    inputs = patches.astype(jnp.float32).reshape(blocks_count, STRIP_DEV, L, D)
    targets = cotangent.astype(jnp.float32).reshape(blocks_count, STRIP_DEV, L, D)
    filled = lengths.astype(jnp.int32).reshape(blocks_count, STRIP_DEV)
    scripts = script.astype(jnp.int32).reshape(blocks_count, STRIP_DEV)

    def advance(carry, item):
        block, target, length_block, script_block = item
        selector = (script_block[:, None] == jnp.arange(GROUPS).astype(jnp.int32)[None, :]).astype(jnp.float32)
        visible = jnp.arange(L).astype(jnp.int32)[None, :] < length_block[:, None]

        def forward(block_in, *weights):
            return layer(block_in, *weights, selector, visible)
        result, pullback = jax.vjp(forward, block, *params)
        grads = pullback(target)
        carry = tuple((total + grad for total, grad in zip(carry, grads[1:])))
        return (carry, (result.astype(jnp.bfloat16), grads[0].astype(jnp.bfloat16)))
    start = tuple((jnp.zeros_like(w) for w in params))
    totals, (results, grad_inputs) = lax.scan(advance, start, (inputs, targets, filled, scripts))
    layer_out = results.reshape(STRIPS, L, D)
    grad_patches = grad_inputs.reshape(STRIPS, L, D)
    return (layer_out, grad_patches, totals[0].T, totals[1], totals[2], totals[3], totals[4], totals[5], totals[6], totals[7], totals[8], totals[9], totals[10], totals[11], totals[12], totals[13])
```

```python
import functools

import jax
import jax.numpy as jnp
from jax import lax
from jax.experimental import pallas as pl
from jax.experimental.pallas import tpu as pltpu
from jax.sharding import PartitionSpec as P

HD = 64


epsilon = 1e-12


def normalize(hidden):
    centred = hidden - jnp.mean(hidden, axis=-1, keepdims=True)
    inverse = lax.rsqrt(jnp.mean(centred * centred, axis=-1, keepdims=True) + epsilon)
    return (centred * inverse, inverse)


def norm_back(upstream, gain, normed, inverse):
    scaled = upstream * gain
    return inverse * (
        scaled
        - jnp.mean(scaled, axis=-1, keepdims=True)
        - normed * jnp.mean(scaled * normed, axis=-1, keepdims=True)
    )


def weight_grad(inputs, upstream):
    return lax.dot_general(
        inputs, upstream, (((0,), (0,)), ((), ())), preferred_element_type=jnp.float32
    )


def input_grad(upstream, weight):
    return lax.dot_general(
        upstream, weight, (((1,), (1,)), ((), ())), preferred_element_type=jnp.float32
    )


def gelu_slope(upper):
    return (
        0.5 * (1.0 + lax.erf(upper * 0.7071067811865476))
        + upper * jnp.exp(-0.5 * upper * upper) * 0.3989422804014327
    )


def split_block(block):
    seq_len = block.shape[0]
    heads_here = block.shape[2] // HD
    return [block[:, member].reshape(seq_len, heads_here, HD) for member in range(3)]


def masked_logits(queries, key_rows, length):
    logits = jnp.einsum(
        "qhd,khd->hqk", queries, key_rows, preferred_element_type=jnp.float32
    ) * HD ** (-0.5)
    visible = jnp.arange(logits.shape[-1], dtype=jnp.int32) < length
    return jnp.where(visible[None, None, :], logits, -1000000000.0)


def attend_forward(item):
    block, length = item
    queries, key_rows, values = split_block(block)
    logits = masked_logits(queries, key_rows, length)
    highest = jnp.max(logits, axis=-1, keepdims=True)
    expanded = jnp.exp(logits - highest)
    totals = jnp.sum(expanded, axis=-1, keepdims=True)
    probs = (expanded / totals).astype(jnp.bfloat16)
    mixed = jnp.einsum("hqk,khd->qhd", probs, values, preferred_element_type=jnp.float32)
    mixed = mixed.astype(jnp.bfloat16).reshape(block.shape[0], block.shape[2])
    return (mixed, (highest + jnp.log(totals))[..., 0])


def attend_backward(item):
    block, log_total, grad_mixed, length = item
    queries, key_rows, values = split_block(block)
    logits = masked_logits(queries, key_rows, length)
    probs = jnp.exp(logits - log_total[..., None])
    grad_heads = grad_mixed.reshape(queries.shape)
    grad_values = jnp.einsum(
        "hqk,qhd->khd", probs.astype(jnp.bfloat16), grad_heads, preferred_element_type=jnp.float32
    )
    grad_probs = jnp.einsum("qhd,khd->hqk", grad_heads, values, preferred_element_type=jnp.float32)
    inner = jnp.sum(probs * grad_probs, axis=-1, keepdims=True)
    grad_logits = (probs * (grad_probs - inner)).astype(jnp.bfloat16)
    grad_queries = jnp.einsum(
        "hqk,khd->qhd", grad_logits, key_rows, preferred_element_type=jnp.float32
    ) * HD ** (-0.5)
    grad_keys = jnp.einsum(
        "hqk,qhd->khd", grad_logits, queries, preferred_element_type=jnp.float32
    ) * HD ** (-0.5)
    stacked = jnp.stack([grad_queries, grad_keys, grad_values], axis=1)
    return stacked.reshape(block.shape).astype(jnp.bfloat16)


def local_general(
    patches,
    lengths,
    script,
    script_table,
    gain_one,
    bias_one,
    qkv_weight,
    query_bias,
    value_bias,
    out_weight,
    out_bias,
    gain_two,
    bias_two,
    up_weight,
    up_bias,
    down_weight,
    down_bias,
    cotangent,
):
    strips, row_count, model_width = patches.shape
    groups = script_table.shape[0]
    tokens = strips * row_count
    selector = (script[:, None] == jnp.arange(groups, dtype=jnp.int32)[None, :]).astype(jnp.float32)
    added = jnp.dot(selector.astype(jnp.bfloat16), script_table, preferred_element_type=jnp.float32)
    hidden = (patches.astype(jnp.float32) + added[:, None, :]).reshape(tokens, model_width)
    normed_one, inverse_one = normalize(hidden)
    inputs_one = (normed_one * gain_one + bias_one).astype(jnp.bfloat16)
    joint_bias = jnp.concatenate([query_bias, jnp.zeros_like(query_bias), value_bias])
    projected = (
        jnp.dot(inputs_one, qkv_weight, preferred_element_type=jnp.float32) + joint_bias
    ).astype(jnp.bfloat16)
    projected = projected.reshape(strips, row_count, 3, model_width)
    head_blocks = lax.all_to_all(projected, "seq", split_axis=3, concat_axis=1, tiled=True)
    mixed_heads, log_totals = lax.map(attend_forward, (head_blocks, lengths))
    mixed = lax.all_to_all(mixed_heads, "seq", split_axis=1, concat_axis=2, tiled=True).reshape(
        tokens, model_width
    )
    attended = hidden + jnp.dot(mixed, out_weight, preferred_element_type=jnp.float32) + out_bias
    normed_two, inverse_two = normalize(attended)
    inputs_two = (normed_two * gain_two + bias_two).astype(jnp.bfloat16)
    upper = jnp.dot(inputs_two, up_weight, preferred_element_type=jnp.float32) + up_bias
    active = jax.nn.gelu(upper, approximate=False).astype(jnp.bfloat16)
    result = attended + jnp.dot(active, down_weight, preferred_element_type=jnp.float32) + down_bias
    layer_out = result.astype(jnp.bfloat16).reshape(strips, row_count, model_width)
    grad_result = cotangent.reshape(tokens, model_width)
    grad_float = grad_result.astype(jnp.float32)
    grad_down_weight = weight_grad(active, grad_result)
    grad_down_bias = jnp.sum(grad_float, axis=0)
    grad_upper = (input_grad(grad_result, down_weight) * gelu_slope(upper)).astype(jnp.bfloat16)
    grad_up_weight = weight_grad(inputs_two, grad_upper)
    grad_up_bias = jnp.sum(grad_upper.astype(jnp.float32), axis=0)
    grad_inputs_two = input_grad(grad_upper, up_weight)
    grad_gain_two = jnp.sum(grad_inputs_two * normed_two, axis=0)
    grad_bias_two = jnp.sum(grad_inputs_two, axis=0)
    grad_attended = grad_float + norm_back(grad_inputs_two, gain_two, normed_two, inverse_two)
    grad_branch = grad_attended.astype(jnp.bfloat16)
    grad_out_weight = weight_grad(mixed, grad_branch)
    grad_out_bias = jnp.sum(grad_branch.astype(jnp.float32), axis=0)
    grad_mixed = (
        input_grad(grad_branch, out_weight)
        .astype(jnp.bfloat16)
        .reshape(strips, row_count, model_width)
    )
    grad_mixed_heads = lax.all_to_all(grad_mixed, "seq", split_axis=2, concat_axis=1, tiled=True)
    grad_heads = lax.map(attend_backward, (head_blocks, log_totals, grad_mixed_heads, lengths))
    grad_projected = lax.all_to_all(
        grad_heads, "seq", split_axis=1, concat_axis=3, tiled=True
    ).reshape(tokens, 3 * model_width)
    grad_qkv = weight_grad(inputs_one, grad_projected)
    grad_bias_rows = jnp.sum(grad_projected.astype(jnp.float32), axis=0)
    grad_query_bias = grad_bias_rows[:model_width]
    grad_value_bias = grad_bias_rows[2 * model_width :]
    grad_inputs_one = input_grad(grad_projected, qkv_weight)
    grad_gain_one = jnp.sum(grad_inputs_one * normed_one, axis=0)
    grad_bias_one = jnp.sum(grad_inputs_one, axis=0)
    grad_hidden = grad_attended + norm_back(grad_inputs_one, gain_one, normed_one, inverse_one)
    grad_patches = grad_hidden.astype(jnp.bfloat16).reshape(strips, row_count, model_width)
    per_strip = jnp.sum(grad_hidden.reshape(strips, row_count, model_width), axis=1)
    grad_table = jnp.dot(per_strip.T, selector, precision=lax.Precision.HIGHEST)
    summed = (
        lax.psum_scatter(grad_table, ("strip", "seq"), scatter_dimension=0, tiled=True),
        lax.psum_scatter(grad_gain_one, ("strip", "seq"), scatter_dimension=0, tiled=True),
        lax.psum_scatter(grad_bias_one, ("strip", "seq"), scatter_dimension=0, tiled=True),
        lax.psum_scatter(grad_qkv, ("strip", "seq"), scatter_dimension=0, tiled=True),
        lax.psum_scatter(grad_query_bias, ("strip", "seq"), scatter_dimension=0, tiled=True),
        lax.psum_scatter(grad_value_bias, ("strip", "seq"), scatter_dimension=0, tiled=True),
        lax.psum_scatter(grad_out_weight, ("strip", "seq"), scatter_dimension=0, tiled=True),
        lax.psum_scatter(grad_out_bias, ("strip", "seq"), scatter_dimension=0, tiled=True),
        lax.psum_scatter(grad_gain_two, ("strip", "seq"), scatter_dimension=0, tiled=True),
        lax.psum_scatter(grad_bias_two, ("strip", "seq"), scatter_dimension=0, tiled=True),
        lax.psum_scatter(grad_up_weight, ("strip", "seq"), scatter_dimension=0, tiled=True),
        lax.psum_scatter(grad_up_bias, ("strip", "seq"), scatter_dimension=0, tiled=True),
        lax.psum_scatter(grad_down_weight, ("strip", "seq"), scatter_dimension=0, tiled=True),
        lax.psum_scatter(grad_down_bias, ("strip", "seq"), scatter_dimension=0, tiled=True),
    )
    return (
        layer_out,
        grad_patches,
        summed[0],
        summed[1],
        summed[2],
        summed[3],
        summed[4],
        summed[5],
        summed[6],
        summed[7],
        summed[8],
        summed[9],
        summed[10],
        summed[11],
        summed[12],
        summed[13],
    )


MESH = pl.DeviceIdType.MESH
BF = jnp.bfloat16
F32 = jnp.float32
CHUNKS = 24
STAGES = 5
WIDE = 384
PART = 24


def small_mesh(mesh):
    return dict(mesh.shape) == {"strip": 8, "seq": 4}


def dot(left, right, left_dim, right_dim):
    return lax.dot_general(
        left, right, (((left_dim,), (right_dim,)), ((), ())), preferred_element_type=F32
    )


def attend_forward_kernel(length_ref, q_ref, k_ref, v_ref, mixed_ref, lse_ref):
    count = q_ref.shape[0]
    lane = lax.broadcasted_iota(jnp.int32, (1, 128), 1)
    visible = lax.broadcasted_iota(jnp.int32, (1, count), 1) < length_ref[0]
    q = q_ref[...] * jnp.asarray(0.125, BF)
    k = k_ref[...]
    v = v_ref[...]
    outs, logs = [], []
    for head in range(2):
        own = (lane // HD) == head
        logits = dot(jnp.where(own, q, jnp.zeros_like(q)), k, 1, 1)
        logits = jnp.where(visible, logits, -1000000000.0)
        highest = jnp.max(logits, axis=1, keepdims=True)
        expanded = jnp.exp(logits - highest)
        total = jnp.sum(expanded, axis=1, keepdims=True)
        probs = (expanded * (1.0 / total)).astype(BF)
        outs.append(dot(probs, v, 1, 0))
        logs.append(highest + jnp.log(total))
    mixed_ref[...] = jnp.where(lane < HD, outs[0], outs[1]).astype(BF)
    lse_ref[...] = jnp.where(lane < HD, logs[0], logs[1])


def attend_backward_kernel(
    length_ref, q_ref, k_ref, v_ref, gm_ref, lse_ref, gq_ref, gk_ref, gv_ref
):
    count = q_ref.shape[0]
    lane = lax.broadcasted_iota(jnp.int32, (1, 128), 1)
    visible = lax.broadcasted_iota(jnp.int32, (1, count), 1) < length_ref[0]
    q = q_ref[...] * jnp.asarray(0.125, BF)
    k = k_ref[...]
    v = v_ref[...]
    gm = gm_ref[...]
    lse = lse_ref[...]
    grads = []
    for head in range(2):
        own = (lane // HD) == head
        q_own = jnp.where(own, q, jnp.zeros_like(q))
        g_own = jnp.where(own, gm, jnp.zeros_like(gm))
        k_own = jnp.where(own, k, jnp.zeros_like(k))
        logits = dot(q_own, k, 1, 1)
        probs = jnp.where(visible, jnp.exp(logits - lse[:, HD * head : HD * head + 1]), 0.0)
        grad_probs = dot(g_own, v, 1, 1)
        inner = jnp.sum(probs * grad_probs, axis=1, keepdims=True)
        grad_logits = (probs * (grad_probs - inner)).astype(BF)
        grads.append(
            (
                dot(grad_logits, k_own, 1, 0),
                dot(q_own, grad_logits, 0, 0),
                dot(g_own, probs.astype(BF), 0, 0),
            )
        )
    gq_ref[...] = ((grads[0][0] + grads[1][0]) * 0.125).astype(BF)
    gk_ref[...] = (grads[0][1] + grads[1][1]).T.astype(BF)
    gv_ref[...] = (grads[0][2] + grads[1][2]).T.astype(BF)


def head_block(count, offset):
    return pl.BlockSpec((count, 128), lambda pair, *_: (0, pair + offset))


def attend_forward_pairs(length, projected):
    count, wide = projected.shape
    pairs = wide // 384
    return pl.pallas_call(
        attend_forward_kernel,
        grid_spec=pltpu.PrefetchScalarGridSpec(
            num_scalar_prefetch=1,
            grid=(pairs,),
            in_specs=[head_block(count, pairs * part) for part in range(3)],
            out_specs=[head_block(count, 0)] * 2,
        ),
        out_shape=[
            jax.ShapeDtypeStruct((count, wide // 3), BF),
            jax.ShapeDtypeStruct((count, wide // 3), F32),
        ],
    )(length, projected, projected, projected)


def attend_backward_pairs(length, projected, grad_mixed, lse):
    count, wide = projected.shape
    pairs = wide // 384
    return pl.pallas_call(
        attend_backward_kernel,
        grid_spec=pltpu.PrefetchScalarGridSpec(
            num_scalar_prefetch=1,
            grid=(pairs,),
            in_specs=[head_block(count, pairs * part) for part in range(3)]
            + [head_block(count, 0)] * 2,
            out_specs=[head_block(count, 0)] * 3,
        ),
        out_shape=[jax.ShapeDtypeStruct((count, wide // 3), BF)] * 3,
    )(length, projected, projected, projected, grad_mixed, lse)


class Reduction:
    def __init__(self, g, r1, r2, r3, r4, s4, r5, out, send, recv):
        self.bufs = (g, r1, r2, r3, r4, s4, r5, out)
        self.sems = (send, recv)
        s, q = lax.axis_index("strip"), lax.axis_index("seq")
        self.s, self.q = s, q
        self.core, self.y = q % 2, q // 2
        self.x, self.low, self.high = s % 2, (s // 2) % 2, s // 4
        self.partners = [
            (s, q + 1 - 2 * self.core),
            (s, q + 2 - 4 * self.y),
            (s + 1 - 2 * self.x, q),
            (s + 2 - 4 * self.low, q),
            (s + 4 - 8 * self.high, q),
        ]

    def side(self, c, second):
        kind = (c + second) % 2
        device = (
            self.s + (1 - kind) * (1 - 2 * self.x),
            self.q + kind * (2 - 4 * self.y),
        )
        return device, (1 - kind) * self.x + kind * self.y

    def copy(self, stage, c):
        g, r1, r2, r3, r4, s4, r5, _ = self.bufs
        if stage == 0:
            source, target, device = g.at[c, 1 - self.core], r1.at[c], self.partners[0]
        elif stage == 1:
            device, bit = self.side(c, 0)
            source, target = r1.at[c, pl.ds((1 - bit) * 192, 192)], r2.at[c]
        elif stage == 2:
            device, bit = self.side(c, 1)
            source, target = r2.at[c, pl.ds((1 - bit) * 96, 96)], r3.at[c]
        elif stage == 3:
            source, target = r3.at[c, pl.ds((1 - self.low) * 48, 48)], r4.at[c]
            device = self.partners[3]
        else:
            source, target = s4.at[c, pl.ds((1 - self.high) * 24, 24)], r5.at[c]
            device = self.partners[4]
        send, recv = self.sems
        return pltpu.make_async_remote_copy(
            src_ref=source,
            dst_ref=target,
            send_sem=send.at[stage, c],
            recv_sem=recv.at[stage, c],
            device_id=device,
            device_id_type=MESH,
        )

    def start(self, c):
        self.copy(0, c).start()

    def event(self, stage, c):
        g, r1, r2, r3, r4, s4, r5, out = self.bufs
        self.copy(stage, c).wait_recv()
        if stage == 0:

            @pl.loop(0, 4)
            def _(i):
                rows = pl.ds(i * 96, 96)
                r1[c, rows] = r1[c, rows] + g[c, self.core, rows]
        elif stage == 1:
            _, bit = self.side(c, 0)

            @pl.loop(0, 2)
            def _(i):
                kept = pl.ds(pl.multiple_of(bit * 192 + i * 96, 96), 96)
                r2[c, pl.ds(i * 96, 96)] = r2[c, pl.ds(i * 96, 96)] + r1[c, kept]
        elif stage == 2:
            _, bit = self.side(c, 1)
            r3[c] = r3[c] + r2[c, pl.ds(pl.multiple_of(bit * 96, 96), 96)]
        elif stage == 3:
            kept = pl.ds(pl.multiple_of(self.low * 48, 48), 48)
            s4[c] = r4[c].astype(F32) + r3[c, kept].astype(F32)
        else:
            out[c] = s4[c, pl.ds(pl.multiple_of(self.high * 24, 24), 24)] + r5[c]
            return
        self.copy(stage + 1, c).start()

    def tick(self, step, lags):
        for stage, lag in enumerate(lags):
            c = step - lag

            @pl.when((c >= 0) & (c < CHUNKS))
            def _():
                self.event(stage, c)

    def finish(self):
        @pl.loop(0, CHUNKS)
        def _(c):
            for stage in range(STAGES):
                self.copy(stage, c).wait_send()


def reduce_vectors(red, vec, recvs, result, send, recv):
    def copy(stage):
        size = 64 >> stage
        bit = (red.core, red.x, red.y, red.low, red.high)[stage]
        device = [red.partners[i] for i in (0, 2, 1, 3, 4)][stage]
        held = vec if stage == 0 else recvs[stage - 1]
        return pltpu.make_async_remote_copy(
            src_ref=held.at[pl.ds((1 - bit) * 2 * size, 2 * size)],
            dst_ref=recvs[stage],
            send_sem=send.at[stage],
            recv_sem=recv.at[stage],
            device_id=device,
            device_id_type=MESH,
        )

    def event(stage):
        size = 64 >> stage
        bit = (red.core, red.x, red.y, red.low, red.high)[stage]
        held = vec if stage == 0 else recvs[stage - 1]
        copy(stage).wait_recv()
        kept = held[pl.ds(pl.multiple_of(bit * 2 * size, 2 * size), 2 * size)]
        if stage < STAGES - 1:
            recvs[stage][...] = recvs[stage][...] + kept
            copy(stage + 1).start()
        else:
            result[...] = recvs[stage][...] + kept

    return copy, event


def gradient_kernel(
    n1, gq, gk, gv, mixed, branch, n2, gupper, active, cot, vec,
    out, vec_out,
    g, r1, r2, r3, r4, s4, r5, product, v1, v2, v3, v4, v5, send, recv, vsend, vrecv,
):
    red = Reduction(g, r1, r2, r3, r4, s4, r5, out, send, recv)
    barrier = pltpu.get_barrier_semaphore()
    for device in red.partners:
        pl.semaphore_signal(barrier, inc=1, device_id=device, device_id_type=MESH)
    pl.semaphore_wait(barrier, len(red.partners))
    vec_copy, vec_event = reduce_vectors(red, vec, (v1, v2, v3, v4, v5), vec_out, vsend, vrecv)
    vec_copy(0).start()
    lags = (2, 4, 6, 8, 10)

    def place(c, row_of):
        kind = c % 2
        for low_owner in range(16):
            core, y, x, low = (
                low_owner % 2, (low_owner // 2) % 2, (low_owner // 4) % 2, low_owner // 8,
            )
            unit = (1 - kind) * (4 * x + 2 * y + low) + kind * (4 * y + 2 * x + low)
            if x == y:
                unit = 4 * x + 2 * y + low
            pair = jnp.concatenate(
                [product[row_of(low_owner)], product[row_of(low_owner + 16)]], axis=0
            )
            where = unit * 48
            if not isinstance(where, int):
                where = pl.multiple_of(where, 48)
            g[c, core, pl.ds(where, 48)] = pair.astype(BF)

    plain = lambda owner: pl.ds(owner * PART, PART)

    @pl.loop(0, 2)
    def _(half):
        columns = pl.ds(pl.multiple_of(half * WIDE, WIDE), WIDE)
        right = cot[:, columns]
        for block in range(4):
            product[pl.ds(block * 768, 768)] = dot(
                active[:, block * 768 : block * 768 + 768], right, 0, 0
            )
        for sub in range(4):
            c = half * 4 + sub
            place(c, lambda owner: pl.ds(owner * 96 + sub * PART, PART))
            red.start(c)
            red.tick(c, lags)

    @pl.loop(8, 16)
    def _(c):
        columns = pl.ds(pl.multiple_of((c - 8) * WIDE, WIDE), WIDE)
        product[pl.ds(0, 768)] = dot(n2[...], gupper[:, columns], 0, 0)
        place(c, plain)
        red.start(c)
        red.tick(c, lags)

    @pl.loop(16, 18)
    def _(c):
        columns = pl.ds(pl.multiple_of((c - 16) * WIDE, WIDE), WIDE)
        product[pl.ds(0, 768)] = dot(mixed[...], branch[:, columns], 0, 0)
        place(c, plain)
        red.start(c)
        red.tick(c, lags)

    for part, grad in enumerate((gq, gk, gv)):

        @pl.loop(18 + 2 * part, 20 + 2 * part)
        def _(c):
            columns = pl.ds(pl.multiple_of((c - 18 - 2 * part) * WIDE, WIDE), WIDE)
            product[pl.ds(0, 768)] = dot(n1[...], grad[:, columns], 0, 0)
            place(c, plain)
            red.start(c)
            red.tick(c, lags)

    for stage in range(STAGES):
        vec_event(stage)

    @pl.loop(CHUNKS, CHUNKS + lags[-1])
    def _(step):
        red.tick(step, lags)

    red.finish()
    for stage in range(STAGES):
        vec_copy(stage).wait_send()


def reduce_gradients(*arrays):
    rows = arrays[0].shape[0]
    whole = pl.BlockSpec(memory_space=pltpu.VMEM)
    return pl.pallas_call(
        gradient_kernel,
        out_shape=[
            jax.ShapeDtypeStruct((CHUNKS, PART, WIDE), F32),
            jax.ShapeDtypeStruct((8, 128), F32),
        ],
        in_specs=[whole] * len(arrays),
        out_specs=[whole] * 2,
        scratch_shapes=[
            pltpu.VMEM((CHUNKS, 2, 384, WIDE), BF),
            pltpu.VMEM((CHUNKS, 384, WIDE), BF),
            pltpu.VMEM((CHUNKS, 192, WIDE), BF),
            pltpu.VMEM((CHUNKS, 96, WIDE), BF),
            pltpu.VMEM((CHUNKS, 48, WIDE), BF),
            pltpu.VMEM((CHUNKS, 48, WIDE), F32),
            pltpu.VMEM((CHUNKS, 24, WIDE), F32),
            pltpu.VMEM((3072, WIDE), F32),
        ]
        + [pltpu.VMEM((128 >> stage, 128), F32) for stage in range(STAGES)]
        + [
            pltpu.SemaphoreType.DMA((STAGES, CHUNKS)),
            pltpu.SemaphoreType.DMA((STAGES, CHUNKS)),
            pltpu.SemaphoreType.DMA((STAGES,)),
            pltpu.SemaphoreType.DMA((STAGES,)),
        ],
        compiler_params=pltpu.CompilerParams(
            collective_id=0, has_side_effects=True, vmem_limit_bytes=60 << 20
        ),
    )(*arrays)


def local(
    patches,
    lengths,
    script,
    script_table,
    gain_one,
    bias_one,
    qkv_weight,
    query_bias,
    value_bias,
    out_weight,
    out_bias,
    gain_two,
    bias_two,
    up_weight,
    up_bias,
    down_weight,
    down_bias,
    cotangent,
):
    strips, row_count, width = patches.shape
    groups = script_table.shape[0]
    tokens = strips * row_count
    mine = lax.axis_index("seq")
    length = lax.dynamic_slice(lengths, (mine,), (1,))
    own_script = lax.dynamic_slice(script, (mine,), (1,))
    selector = (own_script == jnp.arange(groups, dtype=jnp.int32)).astype(F32)
    added = jnp.dot(selector.astype(BF), script_table, preferred_element_type=F32)
    strip_in = lax.all_to_all(patches, "seq", 0, 0, tiled=True).reshape(tokens, width)
    grad_result = lax.all_to_all(cotangent, "seq", 0, 0, tiled=True).reshape(tokens, width)
    hidden = strip_in.astype(F32) + added[None, :]
    normed_one, inverse_one = normalize(hidden)
    inputs_one = (normed_one * gain_one + bias_one).astype(BF)
    joint_bias = jnp.concatenate([query_bias, jnp.zeros_like(query_bias), value_bias])
    projected = (
        jnp.dot(inputs_one, qkv_weight, preferred_element_type=F32) + joint_bias
    ).astype(BF)
    mixed, lse = attend_forward_pairs(length, projected)
    attended = hidden + jnp.dot(mixed, out_weight, preferred_element_type=F32) + out_bias
    normed_two, inverse_two = normalize(attended)
    inputs_two = (normed_two * gain_two + bias_two).astype(BF)
    upper = jnp.dot(inputs_two, up_weight, preferred_element_type=F32) + up_bias
    active = jax.nn.gelu(upper, approximate=False).astype(BF)
    result = attended + jnp.dot(active, down_weight, preferred_element_type=F32) + down_bias
    layer_out = lax.all_to_all(
        result.astype(BF).reshape(strips, row_count, width), "seq", 0, 0, tiled=True
    )
    grad_float = grad_result.astype(F32)
    grad_down_bias = jnp.sum(grad_float, axis=0)
    grad_upper = (input_grad(grad_result, down_weight) * gelu_slope(upper)).astype(BF)
    grad_up_bias = jnp.sum(grad_upper.astype(F32), axis=0)
    grad_inputs_two = input_grad(grad_upper, up_weight)
    grad_gain_two = jnp.sum(grad_inputs_two * normed_two, axis=0)
    grad_bias_two = jnp.sum(grad_inputs_two, axis=0)
    grad_attended = grad_float + norm_back(grad_inputs_two, gain_two, normed_two, inverse_two)
    grad_branch = grad_attended.astype(BF)
    grad_out_bias = jnp.sum(grad_branch.astype(F32), axis=0)
    grad_mixed = input_grad(grad_branch, out_weight).astype(BF)
    grad_q, grad_k, grad_v = attend_backward_pairs(length, projected, grad_mixed, lse)
    grad_query_bias = jnp.sum(grad_q.astype(F32), axis=0)
    grad_value_bias = jnp.sum(grad_v.astype(F32), axis=0)
    grad_inputs_one = (
        input_grad(grad_q, qkv_weight[:, :width])
        + input_grad(grad_k, qkv_weight[:, width : 2 * width])
        + input_grad(grad_v, qkv_weight[:, 2 * width :])
    )
    grad_gain_one = jnp.sum(grad_inputs_one * normed_one, axis=0)
    grad_bias_one = jnp.sum(grad_inputs_one, axis=0)
    grad_hidden = grad_attended + norm_back(grad_inputs_one, gain_one, normed_one, inverse_one)
    grad_patches = lax.all_to_all(
        grad_hidden.astype(BF).reshape(strips, row_count, width), "seq", 0, 0, tiled=True
    )
    grad_table = jnp.sum(grad_hidden, axis=0)[:, None] * selector[None, :]
    owners = 32
    small = [
        grad_gain_one, grad_bias_one, grad_query_bias, grad_value_bias, grad_out_bias,
        grad_gain_two, grad_bias_two, grad_down_bias, grad_up_bias, grad_table,
    ]
    packed = jnp.concatenate([v.reshape(owners, -1) for v in small], axis=1)
    packed = jnp.pad(packed, ((0, 0), (0, 640))).reshape(2, 2, 2, 2, 2, 8, 128)
    packed = packed.transpose(4, 2, 3, 1, 0, 5, 6).reshape(owners * 8, 128)
    reduced, small_sum = reduce_gradients(
        inputs_one, grad_q, grad_k, grad_v, mixed, grad_branch, inputs_two, grad_upper, active,
        grad_result, packed,
    )
    flat = small_sum.reshape(-1)
    part = width // owners
    vectors = [flat[part * i : part * (i + 1)] for i in range(8)]
    up_bias_sum = flat[8 * part : 12 * part]
    table_sum = flat[12 * part : 16 * part].reshape(part, groups)
    down_sum = (
        reduced[0:8].reshape(2, 4, PART, WIDE).transpose(1, 2, 0, 3).reshape(4 * PART, width)
    )
    up_sum = reduced[8:16].transpose(1, 0, 2).reshape(PART, 8 * WIDE)
    out_sum = reduced[16:18].transpose(1, 0, 2).reshape(PART, width)
    qkv_sum = reduced[18:24].transpose(1, 0, 2).reshape(PART, 3 * width)
    return (
        layer_out,
        grad_patches,
        table_sum,
        vectors[0],
        vectors[1],
        qkv_sum,
        vectors[2],
        vectors[3],
        out_sum,
        vectors[4],
        vectors[5],
        vectors[6],
        up_sum,
        up_bias_sum,
        down_sum,
        vectors[7],
    )


def solution(mesh):
    placed = (
        P("strip", "seq", None),
        P("strip"),
        P("strip"),
        P(),
        P(),
        P(),
        P(),
        P(),
        P(),
        P(),
        P(),
        P(),
        P(),
        P(),
        P(),
        P(),
        P(),
        P("strip", "seq", None),
    )
    chosen = local if small_mesh(mesh) else local_general
    return jax.shard_map(
        chosen,
        mesh=mesh,
        in_specs=placed,
        out_specs=(
            P("strip", "seq", None),
            P("strip", "seq", None),
            P(("strip", "seq"), None),
            P(("strip", "seq")),
            P(("strip", "seq")),
            P(("strip", "seq"), None),
            P(("strip", "seq")),
            P(("strip", "seq")),
            P(("strip", "seq"), None),
            P(("strip", "seq")),
            P(("strip", "seq")),
            P(("strip", "seq")),
            P(("strip", "seq"), None),
            P(("strip", "seq")),
            P(("strip", "seq"), None),
            P(("strip", "seq")),
        ),
        check_vma=False,
    )
```

```python
import functools

import jax
import jax.numpy as jnp
from jax import lax
from jax.experimental import pallas as pl
from jax.experimental.pallas import tpu as pltpu
from jax.sharding import PartitionSpec as P

HD = 64


epsilon = 1e-12


def normalize(hidden):
    centred = hidden - jnp.mean(hidden, axis=-1, keepdims=True)
    inverse = lax.rsqrt(jnp.mean(centred * centred, axis=-1, keepdims=True) + epsilon)
    return (centred * inverse, inverse)


def norm_back(upstream, gain, normed, inverse):
    scaled = upstream * gain
    return inverse * (
        scaled
        - jnp.mean(scaled, axis=-1, keepdims=True)
        - normed * jnp.mean(scaled * normed, axis=-1, keepdims=True)
    )


def weight_grad(inputs, upstream):
    return lax.dot_general(
        inputs, upstream, (((0,), (0,)), ((), ())), preferred_element_type=jnp.float32
    )


def input_grad(upstream, weight):
    return lax.dot_general(
        upstream, weight, (((1,), (1,)), ((), ())), preferred_element_type=jnp.float32
    )


def gelu_slope(upper):
    return (
        0.5 * (1.0 + lax.erf(upper * 0.7071067811865476))
        + upper * jnp.exp(-0.5 * upper * upper) * 0.3989422804014327
    )


def split_block(block):
    seq_len = block.shape[0]
    heads_here = block.shape[2] // HD
    return [block[:, member].reshape(seq_len, heads_here, HD) for member in range(3)]


def masked_logits(queries, key_rows, length):
    logits = jnp.einsum(
        "qhd,khd->hqk", queries, key_rows, preferred_element_type=jnp.float32
    ) * HD ** (-0.5)
    visible = jnp.arange(logits.shape[-1], dtype=jnp.int32) < length
    return jnp.where(visible[None, None, :], logits, -1000000000.0)


def attend_forward(item):
    block, length = item
    queries, key_rows, values = split_block(block)
    logits = masked_logits(queries, key_rows, length)
    highest = jnp.max(logits, axis=-1, keepdims=True)
    expanded = jnp.exp(logits - highest)
    totals = jnp.sum(expanded, axis=-1, keepdims=True)
    probs = (expanded / totals).astype(jnp.bfloat16)
    mixed = jnp.einsum("hqk,khd->qhd", probs, values, preferred_element_type=jnp.float32)
    mixed = mixed.astype(jnp.bfloat16).reshape(block.shape[0], block.shape[2])
    return (mixed, (highest + jnp.log(totals))[..., 0])


def attend_backward(item):
    block, log_total, grad_mixed, length = item
    queries, key_rows, values = split_block(block)
    logits = masked_logits(queries, key_rows, length)
    probs = jnp.exp(logits - log_total[..., None])
    grad_heads = grad_mixed.reshape(queries.shape)
    grad_values = jnp.einsum(
        "hqk,qhd->khd", probs.astype(jnp.bfloat16), grad_heads, preferred_element_type=jnp.float32
    )
    grad_probs = jnp.einsum("qhd,khd->hqk", grad_heads, values, preferred_element_type=jnp.float32)
    inner = jnp.sum(probs * grad_probs, axis=-1, keepdims=True)
    grad_logits = (probs * (grad_probs - inner)).astype(jnp.bfloat16)
    grad_queries = jnp.einsum(
        "hqk,khd->qhd", grad_logits, key_rows, preferred_element_type=jnp.float32
    ) * HD ** (-0.5)
    grad_keys = jnp.einsum(
        "hqk,qhd->khd", grad_logits, queries, preferred_element_type=jnp.float32
    ) * HD ** (-0.5)
    stacked = jnp.stack([grad_queries, grad_keys, grad_values], axis=1)
    return stacked.reshape(block.shape).astype(jnp.bfloat16)


def local_general(
    patches,
    lengths,
    script,
    script_table,
    gain_one,
    bias_one,
    qkv_weight,
    query_bias,
    value_bias,
    out_weight,
    out_bias,
    gain_two,
    bias_two,
    up_weight,
    up_bias,
    down_weight,
    down_bias,
    cotangent,
):
    strips, row_count, model_width = patches.shape
    groups = script_table.shape[0]
    tokens = strips * row_count
    selector = (script[:, None] == jnp.arange(groups, dtype=jnp.int32)[None, :]).astype(jnp.float32)
    added = jnp.dot(selector.astype(jnp.bfloat16), script_table, preferred_element_type=jnp.float32)
    hidden = (patches.astype(jnp.float32) + added[:, None, :]).reshape(tokens, model_width)
    normed_one, inverse_one = normalize(hidden)
    inputs_one = (normed_one * gain_one + bias_one).astype(jnp.bfloat16)
    joint_bias = jnp.concatenate([query_bias, jnp.zeros_like(query_bias), value_bias])
    projected = (
        jnp.dot(inputs_one, qkv_weight, preferred_element_type=jnp.float32) + joint_bias
    ).astype(jnp.bfloat16)
    projected = projected.reshape(strips, row_count, 3, model_width)
    head_blocks = lax.all_to_all(projected, "seq", split_axis=3, concat_axis=1, tiled=True)
    mixed_heads, log_totals = lax.map(attend_forward, (head_blocks, lengths))
    mixed = lax.all_to_all(mixed_heads, "seq", split_axis=1, concat_axis=2, tiled=True).reshape(
        tokens, model_width
    )
    attended = hidden + jnp.dot(mixed, out_weight, preferred_element_type=jnp.float32) + out_bias
    normed_two, inverse_two = normalize(attended)
    inputs_two = (normed_two * gain_two + bias_two).astype(jnp.bfloat16)
    upper = jnp.dot(inputs_two, up_weight, preferred_element_type=jnp.float32) + up_bias
    active = jax.nn.gelu(upper, approximate=False).astype(jnp.bfloat16)
    result = attended + jnp.dot(active, down_weight, preferred_element_type=jnp.float32) + down_bias
    layer_out = result.astype(jnp.bfloat16).reshape(strips, row_count, model_width)
    grad_result = cotangent.reshape(tokens, model_width)
    grad_float = grad_result.astype(jnp.float32)
    grad_down_weight = weight_grad(active, grad_result)
    grad_down_bias = jnp.sum(grad_float, axis=0)
    grad_upper = (input_grad(grad_result, down_weight) * gelu_slope(upper)).astype(jnp.bfloat16)
    grad_up_weight = weight_grad(inputs_two, grad_upper)
    grad_up_bias = jnp.sum(grad_upper.astype(jnp.float32), axis=0)
    grad_inputs_two = input_grad(grad_upper, up_weight)
    grad_gain_two = jnp.sum(grad_inputs_two * normed_two, axis=0)
    grad_bias_two = jnp.sum(grad_inputs_two, axis=0)
    grad_attended = grad_float + norm_back(grad_inputs_two, gain_two, normed_two, inverse_two)
    grad_branch = grad_attended.astype(jnp.bfloat16)
    grad_out_weight = weight_grad(mixed, grad_branch)
    grad_out_bias = jnp.sum(grad_branch.astype(jnp.float32), axis=0)
    grad_mixed = (
        input_grad(grad_branch, out_weight)
        .astype(jnp.bfloat16)
        .reshape(strips, row_count, model_width)
    )
    grad_mixed_heads = lax.all_to_all(grad_mixed, "seq", split_axis=2, concat_axis=1, tiled=True)
    grad_heads = lax.map(attend_backward, (head_blocks, log_totals, grad_mixed_heads, lengths))
    grad_projected = lax.all_to_all(
        grad_heads, "seq", split_axis=1, concat_axis=3, tiled=True
    ).reshape(tokens, 3 * model_width)
    grad_qkv = weight_grad(inputs_one, grad_projected)
    grad_bias_rows = jnp.sum(grad_projected.astype(jnp.float32), axis=0)
    grad_query_bias = grad_bias_rows[:model_width]
    grad_value_bias = grad_bias_rows[2 * model_width :]
    grad_inputs_one = input_grad(grad_projected, qkv_weight)
    grad_gain_one = jnp.sum(grad_inputs_one * normed_one, axis=0)
    grad_bias_one = jnp.sum(grad_inputs_one, axis=0)
    grad_hidden = grad_attended + norm_back(grad_inputs_one, gain_one, normed_one, inverse_one)
    grad_patches = grad_hidden.astype(jnp.bfloat16).reshape(strips, row_count, model_width)
    per_strip = jnp.sum(grad_hidden.reshape(strips, row_count, model_width), axis=1)
    grad_table = jnp.dot(per_strip.T, selector, precision=lax.Precision.HIGHEST)
    summed = (
        lax.psum_scatter(grad_table, ("strip", "seq"), scatter_dimension=0, tiled=True),
        lax.psum_scatter(grad_gain_one, ("strip", "seq"), scatter_dimension=0, tiled=True),
        lax.psum_scatter(grad_bias_one, ("strip", "seq"), scatter_dimension=0, tiled=True),
        lax.psum_scatter(grad_qkv, ("strip", "seq"), scatter_dimension=0, tiled=True),
        lax.psum_scatter(grad_query_bias, ("strip", "seq"), scatter_dimension=0, tiled=True),
        lax.psum_scatter(grad_value_bias, ("strip", "seq"), scatter_dimension=0, tiled=True),
        lax.psum_scatter(grad_out_weight, ("strip", "seq"), scatter_dimension=0, tiled=True),
        lax.psum_scatter(grad_out_bias, ("strip", "seq"), scatter_dimension=0, tiled=True),
        lax.psum_scatter(grad_gain_two, ("strip", "seq"), scatter_dimension=0, tiled=True),
        lax.psum_scatter(grad_bias_two, ("strip", "seq"), scatter_dimension=0, tiled=True),
        lax.psum_scatter(grad_up_weight, ("strip", "seq"), scatter_dimension=0, tiled=True),
        lax.psum_scatter(grad_up_bias, ("strip", "seq"), scatter_dimension=0, tiled=True),
        lax.psum_scatter(grad_down_weight, ("strip", "seq"), scatter_dimension=0, tiled=True),
        lax.psum_scatter(grad_down_bias, ("strip", "seq"), scatter_dimension=0, tiled=True),
    )
    return (
        layer_out,
        grad_patches,
        summed[0],
        summed[1],
        summed[2],
        summed[3],
        summed[4],
        summed[5],
        summed[6],
        summed[7],
        summed[8],
        summed[9],
        summed[10],
        summed[11],
        summed[12],
        summed[13],
    )


MESH = pl.DeviceIdType.MESH
BF = jnp.bfloat16
F32 = jnp.float32
CHUNKS = 24
SLOTS = 12
STAGES = 5
WIDE = 384
PART = 24
BLOCK = 32
LAGS = (2, 5, 7, 9, 11)


def fits(mesh):
    return dict(mesh.shape) == {"strip": 8, "seq": 4}


def dot(left, right, left_dim, right_dim):
    return lax.dot_general(
        left, right, (((left_dim,), (right_dim,)), ((), ())), preferred_element_type=F32
    )


def mean(block):
    return jnp.mean(block, axis=1, keepdims=True)


def fold(block):
    return jnp.sum(block.reshape(block.shape[0] // 8, 8, block.shape[1]), axis=0)


def column_sum(block):
    return jnp.sum(block, axis=0, keepdims=True)


def attend_pair(pair, length, proj, mixed, lse_all):
    count = proj.shape[0]
    width = proj.shape[1] // 3
    at = lambda part: pl.ds(pl.multiple_of(part * width + pair * 128, 128), 128)
    lane = lax.broadcasted_iota(jnp.int32, (1, 128), 1)
    visible = lax.broadcasted_iota(jnp.int32, (1, count), 1) < length
    q = proj[:, at(0)] * jnp.asarray(0.125, BF)
    k = proj[:, at(1)]
    v = proj[:, at(2)]
    outs, logs = [], []
    for head in range(2):
        own = (lane // HD) == head
        logits = dot(jnp.where(own, q, jnp.zeros_like(q)), k, 1, 1)
        logits = jnp.where(visible, logits, -1000000000.0)
        highest = jnp.max(logits, axis=1, keepdims=True)
        expanded = jnp.exp(logits - highest)
        total = jnp.sum(expanded, axis=1, keepdims=True)
        probs = (expanded * (1.0 / total)).astype(BF)
        outs.append(dot(probs, v, 1, 0))
        logs.append(highest + jnp.log(total))
    mixed[:, at(0)] = jnp.where(lane < HD, outs[0], outs[1]).astype(BF)
    known = jnp.where(lane == 2 * pair, logs[0], lse_all[...])
    lse_all[...] = jnp.where(lane == 2 * pair + 1, logs[1], known)


def attend_pair_back(pair, length, proj, gmixed, lse_all):
    count = proj.shape[0]
    width = proj.shape[1] // 3
    at = lambda part: pl.ds(pl.multiple_of(part * width + pair * 128, 128), 128)
    lane = lax.broadcasted_iota(jnp.int32, (1, 128), 1)
    visible = lax.broadcasted_iota(jnp.int32, (1, count), 1) < length
    q = proj[:, at(0)] * jnp.asarray(0.125, BF)
    k = proj[:, at(1)]
    v = proj[:, at(2)]
    gm = gmixed[:, at(0)]
    lse = lse_all[...]
    grads = []
    for head in range(2):
        own = (lane // HD) == head
        q_own = jnp.where(own, q, jnp.zeros_like(q))
        g_own = jnp.where(own, gm, jnp.zeros_like(gm))
        k_own = jnp.where(own, k, jnp.zeros_like(k))
        own_lse = jnp.sum(jnp.where(lane == 2 * pair + head, lse, 0.0), axis=1, keepdims=True)
        logits = dot(q_own, k, 1, 1)
        probs = jnp.where(visible, jnp.exp(logits - own_lse), 0.0)
        grad_probs = dot(g_own, v, 1, 1)
        inner = jnp.sum(probs * grad_probs, axis=1, keepdims=True)
        grad_logits = (probs * (grad_probs - inner)).astype(BF)
        grads.append(
            (
                dot(grad_logits, k_own, 1, 0),
                dot(q_own, grad_logits, 0, 0),
                dot(g_own, probs.astype(BF), 0, 0),
            )
        )
    gq = ((grads[0][0] + grads[1][0]) * 0.125).astype(BF)
    gk = (grads[0][1] + grads[1][1]).T.astype(BF)
    gv = (grads[0][2] + grads[1][2]).T.astype(BF)
    return gq, gk, gv


class Devices:
    def __init__(self):
        s, q = lax.axis_index("strip"), lax.axis_index("seq")
        self.s, self.q = s, q
        self.core, self.y = q % 2, q // 2
        self.x, self.low, self.high = s % 2, (s // 2) % 2, s // 4
        self.to_core = (s, q + 1 - 2 * self.core)
        self.to_y = (s, q + 2 - 4 * self.y)
        self.to_x = (s + 1 - 2 * self.x, q)
        self.to_low = (s + 2 - 4 * self.low, q)
        self.to_high = (s + 4 - 8 * self.high, q)


def kinds(c):
    kind = c % 3
    return (2 - kind) * (1 - kind) // 2, kind * (2 - kind), kind * (kind - 1) // 2


class Reduction:
    def __init__(self, dev, g, r1, r2, r3, r4, s4, r5, write, send, recv):
        self.dev = dev
        self.bufs = (g, r1, r2, r3, r4, s4, r5)
        self.write = write
        self.sems = (send, recv)

    def side(self, stage, c):
        dev = self.dev
        in_x, in_y, in_z = kinds(c)
        if stage == 1:
            by_x, by_y, by_low = in_x, in_y, in_z
        elif stage == 2:
            by_x, by_y, by_low = in_y + in_z, in_x, 0
        else:
            by_x, by_y, by_low = 0, in_z, in_x + in_y
        device = (
            dev.s + by_x * (1 - 2 * dev.x) + by_low * (2 - 4 * dev.low),
            dev.q + by_y * (2 - 4 * dev.y),
        )
        return device, by_x * dev.x + by_y * dev.y + by_low * dev.low

    def copy(self, stage, c):
        g, r1, r2, r3, r4, s4, r5 = self.bufs
        dev = self.dev
        if stage == 0:
            source, target, device = g.at[c % SLOTS, 1 - dev.core], r1.at[c], dev.to_core
        elif stage == 4:
            source, target = s4.at[c, pl.ds((1 - dev.high) * 24, 24)], r5.at[c]
            device = dev.to_high
        else:
            device, bit = self.side(stage, c)
            rows = 384 >> stage
            held, target = ((r1, r2), (r2, r3), (r3, r4))[stage - 1]
            source, target = held.at[c, pl.ds((1 - bit) * rows, rows)], target.at[c]
        send, recv = self.sems
        return pltpu.make_async_remote_copy(
            src_ref=source,
            dst_ref=target,
            send_sem=send.at[stage, c],
            recv_sem=recv.at[stage, c],
            device_id=device,
            device_id_type=MESH,
        )

    def free(self, c):
        @pl.when(c >= SLOTS)
        def _():
            self.copy(0, c - SLOTS).wait_send()

    def start(self, c):
        self.copy(0, c).start()

    def event(self, stage, c):
        g, r1, r2, r3, r4, s4, r5 = self.bufs
        dev = self.dev
        self.copy(stage, c).wait_recv()
        if stage == 0:

            @pl.loop(0, 4)
            def _(i):
                rows = pl.ds(i * 96, 96)
                r1[c, rows] = r1[c, rows] + g[c % SLOTS, dev.core, rows]
        elif stage < 3:
            _, bit = self.side(stage, c)
            held, target = ((r1, r2), (r2, r3))[stage - 1]

            @pl.loop(0, 4 >> stage)
            def _(i):
                rows = pl.ds(i * 96, 96)
                kept = pl.ds(pl.multiple_of(bit * (384 >> stage) + i * 96, 96), 96)
                target[c, rows] = target[c, rows] + held[c, kept]
        elif stage == 3:
            _, bit = self.side(stage, c)
            kept = pl.ds(pl.multiple_of(bit * 48, 48), 48)
            s4[c] = r4[c].astype(F32) + r3[c, kept].astype(F32)
        else:
            self.write[c] = s4[c, pl.ds(pl.multiple_of(dev.high * 24, 24), 24)] + r5[c]
            return
        self.copy(stage + 1, c).start()

    def tick(self, step):
        for stage, lag in enumerate(LAGS):
            c = step - lag

            @pl.when((c >= 0) & (c < CHUNKS))
            def _():
                self.event(stage, c)

    def finish(self):
        @pl.loop(0, CHUNKS)
        def _(c):
            for stage in range(1, STAGES):
                self.copy(stage, c).wait_send()

        @pl.loop(CHUNKS - SLOTS, CHUNKS)
        def _(c):
            self.copy(0, c).wait_send()

    def put(self, c, core, x, y, low, rows):
        in_x, in_y, in_z = kinds(c)
        unit = (
            in_x * (4 * x + 2 * y + low)
            + in_y * (4 * y + 2 * x + low)
            + in_z * (4 * low + 2 * x + y)
        )
        where = unit * 48
        if not isinstance(where, int):
            where = pl.multiple_of(where, 48)
        self.bufs[0][c % SLOTS, core, pl.ds(where, 48)] = rows.astype(BF)

    def place(self, c, half, product):
        columns = pl.ds(half * WIDE, WIDE)
        for owner in range(16):
            pair = jnp.concatenate(
                [
                    product[pl.ds(owner * PART, PART), columns],
                    product[pl.ds((owner + 16) * PART, PART), columns],
                ],
                axis=0,
            )
            self.put(c, owner % 2, (owner // 4) % 2, (owner // 2) % 2, owner // 8, pair)


ERF_TOP = (
    0.00022905065861350646, 0.0034082910107109506, 0.050955695062380861, 0.18520832239976145,
    1.128379143519084,
)
ERF_BOTTOM = (
    -1.1791602954361697e-7, 0.000023547966471313185, 0.0010179625278914885,
    0.014070470171167667, 0.11098505178285362, 0.49746925110067538, 1.0,
)


def erf(value):
    value = jnp.clip(value, -3.832506856900711, 3.832506856900711)
    square = value * value
    top = jnp.full_like(square, ERF_TOP[0])
    for term in ERF_TOP[1:]:
        top = top * square + term
    bottom = jnp.full_like(square, ERF_BOTTOM[0])
    for term in ERF_BOTTOM[1:]:
        bottom = bottom * square + term
    return value * top / bottom


def standardize(block):
    centred = block - mean(block)
    inverse = lax.rsqrt(mean(centred * centred) + epsilon)
    return centred * inverse, inverse


def layer_kernel(
    lengths, script, table, gain_one, bias_one, query_bias, value_bias, out_bias, gain_two,
    bias_two, up_bias, down_bias, patches, cotangent, qkv_hbm, out_hbm, up_hbm, down_hbm,
    layer_out, grad_patches, reduced, small,
    xin, cin, hidden, n1, proj, mixed, lse_all, att, n2, active, cot, res, gn, branch, gmixed,
    gblk, product, jbias, vecs, wqkv, wout, wup, wdown,
    g, r1, r2, r3, r4, s4, r5, v1, v2, v3, v4, v5,
    send, recv, vsend, vrecv, xsend, xrecv, wsem, fsem, osem,
):
    strips, row_count, width = patches.shape
    count = strips * row_count
    rows = hidden.shape[0]
    blocks = rows // BLOCK
    ff_blocks = up_hbm.shape[1] // width
    dev = Devices()
    s, q = dev.s, dev.q
    red = Reduction(dev, g, r1, r2, r3, r4, s4, r5, reduced, send, recv)

    barrier = pltpu.get_barrier_semaphore()
    greeted = [(s, (q + hop) % strips) for hop in range(1, strips)]
    greeted += [dev.to_x, dev.to_low, dev.to_high]
    for device in greeted:
        pl.semaphore_signal(barrier, inc=1, device_id=device, device_id_type=MESH)

    load_qkv = pltpu.make_async_copy(qkv_hbm, wqkv, wsem.at[0])
    load_out = pltpu.make_async_copy(out_hbm, wout, wsem.at[1])

    def load_ff(block):
        columns = pl.ds(pl.multiple_of(block * width, width), width)
        slot = block % 2
        return (
            pltpu.make_async_copy(up_hbm.at[:, columns], wup.at[slot], fsem.at[0, slot]),
            pltpu.make_async_copy(down_hbm.at[columns], wdown.at[slot], fsem.at[1, slot]),
        )

    def exchange(group, source, target):
        copies = []
        for hop in range(1, strips):
            other = (q + hop) % strips
            copies.append(
                pltpu.make_async_remote_copy(
                    src_ref=source.at[other],
                    dst_ref=target.at[q],
                    send_sem=xsend.at[group, hop],
                    recv_sem=xrecv.at[group, hop],
                    device_id=(s, other),
                    device_id_type=MESH,
                )
            )
        own = pltpu.make_async_copy(source.at[q], target.at[q], osem.at[group])
        return copies, own

    def launch(moves):
        copies, own = moves
        for index in (1, 0, 2):
            copies[index].start()
        own.start()

    def arrive(moves):
        copies, own = moves
        for copy in copies:
            copy.wait_recv()
        own.wait()

    into_x = exchange(0, patches, xin)
    into_c = exchange(1, cotangent, cin)
    pl.semaphore_wait(barrier, len(greeted))
    launch(into_x)
    load_qkv.start()
    load_out.start()
    for copy in load_ff(0):
        copy.start()
    launch(into_c)

    length = lengths[q]
    own_script = script[q]
    added = jnp.zeros((1, width), F32)
    for group in range(table.shape[0]):
        added = jnp.where(own_script == group, table[pl.ds(group, 1)].astype(F32), added)
    row = lambda ref: ref[...].reshape(1, ref.shape[0])
    jbias[pl.ds(0, 1)] = row(query_bias)
    jbias[pl.ds(1, 1)] = jnp.zeros((1, width), F32)
    jbias[pl.ds(2, 1)] = row(value_bias)
    hidden[pl.ds(count, rows - count)] = jnp.zeros((rows - count, width), F32)
    gn[pl.ds(count, rows - count)] = jnp.zeros((rows - count, width), F32)
    lse_all[...] = jnp.zeros_like(lse_all)

    arrive(into_x)
    for j in range(strips):
        hidden[pl.ds(j * row_count, row_count)] = xin[j].astype(F32) + added

    @pl.loop(0, blocks)
    def _(b):
        at = pl.ds(pl.multiple_of(b * BLOCK, BLOCK), BLOCK)
        normed, _ = standardize(hidden[at])
        n1[at] = (normed * row(gain_one) + row(bias_one)).astype(BF)

    load_qkv.wait()

    @pl.loop(0, 3)
    def _(part):
        columns = pl.ds(pl.multiple_of(part * width, width), width)
        proj[:, columns] = (dot(n1[...], wqkv[:, columns], 1, 0) + jbias[pl.ds(part, 1)]).astype(BF)

    @pl.loop(0, width // 128)
    def _(pair):
        attend_pair(pair, length, proj, mixed, lse_all)

    arrive(into_c)
    for j in range(strips):
        gn[pl.ds(j * row_count, row_count)] = cin[j].astype(F32)
    load_out.wait()
    att[...] = hidden[...] + dot(mixed[...], wout[...], 1, 0) + row(out_bias)
    zero8 = jnp.zeros((8, width), F32)

    def second_norm(b, total):
        at = pl.ds(pl.multiple_of(b * BLOCK, BLOCK), BLOCK)
        block = att[at]
        normed, _ = standardize(block)
        n2[at] = (normed * row(gain_two) + row(bias_two)).astype(BF)
        res[at] = block + row(down_bias)
        upstream = gn[at]
        cot[at] = upstream.astype(BF)
        gn[at] = jnp.zeros((BLOCK, width), F32)
        return total + fold(upstream)

    vecs[pl.ds(7, 1)] = column_sum(lax.fori_loop(0, blocks, second_norm, zero8))

    @pl.loop(0, ff_blocks)
    def _(block):
        slot = block % 2
        for copy in load_ff(block):
            copy.wait()

        @pl.when(block + 1 < ff_blocks)
        def _():
            for copy in load_ff(block + 1):
                copy.start()

        up = wup[slot]
        down = wdown[slot]
        upper = dot(n2[...], up, 1, 0) + up_bias[pl.ds(block, 1)]
        grad_active = dot(cot[...], down, 1, 1)
        share = 0.5 * (1.0 + erf(upper * 0.7071067811865476))
        columns = pl.ds(pl.multiple_of(block * width, width), width)
        act = (upper * share).astype(BF)
        active[:, columns] = act
        slope = share + upper * jnp.exp(-0.5 * upper * upper) * 0.3989422804014327
        grad_upper = (grad_active * slope).astype(BF)
        gblk[...] = grad_upper
        res[...] += dot(act, down, 1, 0)
        gn[...] += dot(grad_upper, up, 1, 1)
        vecs[pl.ds(12 + block, 1)] = column_sum(grad_upper.astype(F32))
        product[...] = dot(n2[...], gblk[...], 0, 0)
        for half in range(2):
            c = 2 * block + half
            red.free(c)
            red.place(c, half, product)
            red.start(c)
            red.tick(c)

    for j in range(strips):
        xin[j] = res[pl.ds(j * row_count, row_count)].astype(BF)
    from_out = exchange(2, xin, layer_out)
    launch(from_out)

    def second_back(b, totals):
        at = pl.ds(pl.multiple_of(b * BLOCK, BLOCK), BLOCK)
        normed, inverse = standardize(att[at])
        upstream = gn[at]
        scaled = upstream * row(gain_two)
        back = inverse * (scaled - mean(scaled) - normed * mean(scaled * normed))
        grad = cot[at].astype(F32) + back
        rounded = grad.astype(BF)
        gn[at] = grad
        branch[at] = rounded
        return (
            totals[0] + fold(upstream * normed),
            totals[1] + fold(upstream),
            totals[2] + fold(rounded.astype(F32)),
        )

    totals = lax.fori_loop(0, blocks, second_back, (zero8, zero8, zero8))
    vecs[pl.ds(5, 1)] = column_sum(totals[0])
    vecs[pl.ds(6, 1)] = column_sum(totals[1])
    vecs[pl.ds(4, 1)] = column_sum(totals[2])
    gmixed[...] = dot(branch[...], wout[...], 1, 1).astype(BF)
    product[...] = dot(mixed[...], branch[...], 0, 0)
    for half in range(2):
        c = 8 + half
        red.free(c)
        red.place(c, half, product)
        red.start(c)
        red.tick(c)

    @pl.loop(10, 18)
    def _(c):
        red.free(c)

    @pl.loop(0, 4)
    def _(b):
        left = jnp.concatenate(
            [
                active[:, pl.ds(pl.multiple_of(b * WIDE, WIDE), WIDE)],
                active[:, pl.ds(pl.multiple_of(4 * WIDE + b * WIDE, WIDE), WIDE)],
            ],
            axis=1,
        )
        product[...] = dot(left, cot[...], 0, 0)
        for half in range(2):
            for sub in range(4):
                for near in range(4):
                    at = near * 4 * PART + sub * PART
                    columns = pl.ds(half * WIDE, WIDE)
                    pair = jnp.concatenate(
                        [
                            product[pl.ds(at, PART), columns],
                            product[pl.ds(at + 384, PART), columns],
                        ],
                        axis=0,
                    )
                    red.put(10 + 4 * half + sub, near % 2, b % 2, near // 2, b // 2, pair)

    @pl.loop(10, 18)
    def _(c):
        red.start(c)

    res[...] = jnp.zeros_like(res)

    @pl.loop(0, 3)
    def _(i):
        @pl.loop(0, 2)
        def _(h):
            pair = 2 * i + h
            grads = attend_pair_back(pair, length, proj, gmixed, lse_all)
            for part in range(3):
                gblk[:, pl.ds(pl.multiple_of(h * WIDE + part * 128, 128), 128)] = grads[part]
            lanes = pl.ds(pl.multiple_of(pair * 128, 128), 128)
            vecs[pl.ds(2, 1), lanes] = column_sum(grads[0].astype(F32))
            vecs[pl.ds(3, 1), lanes] = column_sum(grads[2].astype(F32))

            @pl.loop(0, 2)
            def _(k):
                red.tick(10 + 5 * i + 2 * h + k)

        product[...] = dot(n1[...], gblk[...], 0, 0)
        for half in range(2):
            c = 18 + 2 * i + half
            red.free(c)
            red.place(c, half, product)
            red.start(c)
        red.tick(14 + 5 * i)
        weights = jnp.concatenate(
            [
                wqkv[:, pl.ds(pl.multiple_of(part * width + (2 * i + h) * 128, 128), 128)]
                for h in range(2)
                for part in range(3)
            ],
            axis=1,
        )
        res[...] += dot(gblk[...], weights, 1, 1)

    def first_back(b, totals):
        at = pl.ds(pl.multiple_of(b * BLOCK, BLOCK), BLOCK)
        normed, inverse = standardize(hidden[at])
        upstream = res[at]
        scaled = upstream * row(gain_one)
        back = inverse * (scaled - mean(scaled) - normed * mean(scaled * normed))
        grad = gn[at] + back
        res[at] = grad
        return (
            totals[0] + fold(upstream * normed),
            totals[1] + fold(upstream),
            totals[2] + fold(grad),
        )

    totals = lax.fori_loop(0, blocks, first_back, (zero8, zero8, zero8))
    vecs[pl.ds(0, 1)] = column_sum(totals[0])
    vecs[pl.ds(1, 1)] = column_sum(totals[1])
    strip_sum = column_sum(totals[2])
    for group in range(table.shape[0]):
        vecs[pl.ds(8 + group, 1)] = jnp.where(own_script == group, strip_sum, 0.0)
    for j in range(strips):
        cin[j] = res[pl.ds(j * row_count, row_count)].astype(BF)
    from_grad = exchange(3, cin, grad_patches)
    launch(from_grad)

    held = (vecs, v1, v2, v3, v4, v5)
    order = (dev.to_core, dev.to_x, dev.to_y, dev.to_low, dev.to_high)

    def share_copy(stage):
        return pltpu.make_async_remote_copy(
            src_ref=held[stage],
            dst_ref=held[stage + 1],
            send_sem=vsend.at[stage],
            recv_sem=vrecv.at[stage],
            device_id=order[stage],
            device_id_type=MESH,
        )

    share_copy(0).start()
    done = 25
    for stage in range(STAGES):
        upto = CHUNKS + LAGS[min(stage, STAGES - 1)]

        @pl.loop(done, upto)
        def _(step):
            red.tick(step)

        done = max(done, upto)
        share_copy(stage).wait_recv()
        held[stage + 1][...] = held[stage + 1][...] + held[stage][...]
        if stage + 1 < STAGES:
            share_copy(stage + 1).start()

    owner = s * strips + q
    spread = lax.broadcasted_iota(jnp.int32, (width, 128), 0)
    lane = lax.broadcasted_iota(jnp.int32, (width, 128), 1)
    few = jnp.where((spread == PART * owner + lane) & (lane < PART), 1.0, 0.0)
    many = jnp.where((spread == 4 * PART * (owner % 8) + lane) & (lane < 4 * PART), 1.0, 0.0)
    exact = lambda left, right: lax.dot_general(
        left, right, (((1,), (0,)), ((), ())), precision=lax.Precision.HIGHEST,
        preferred_element_type=F32,
    )
    summed = v5[...]
    lines = lax.broadcasted_iota(jnp.int32, (16, width), 0)
    chosen = jnp.where(lines == 12 + owner // 8, summed, 0.0)
    small[pl.ds(0, 16)] = exact(summed, few)
    small[pl.ds(16, 16)] = exact(chosen, many)

    red.finish()
    for stage in range(STAGES):
        share_copy(stage).wait_send()
    for moves in (from_out, from_grad):
        arrive(moves)
    for moves in (into_x, into_c, from_out, from_grad):
        for copy in moves[0]:
            copy.wait_send()


def run_layer(*arrays):
    patches = arrays[12]
    strips, row_count, width = patches.shape
    rows = -(-strips * row_count // BLOCK) * BLOCK
    hidden_units = arrays[16].shape[1]
    vmem = pl.BlockSpec(memory_space=pltpu.VMEM)
    smem = pl.BlockSpec(memory_space=pltpu.SMEM)
    hbm = pl.BlockSpec(memory_space=pl.ANY)
    packed = lambda *shape: pltpu.VMEM(shape, BF)
    wide = lambda *shape: pltpu.VMEM(shape, F32)
    return pl.pallas_call(
        layer_kernel,
        out_shape=[
            jax.ShapeDtypeStruct(patches.shape, BF),
            jax.ShapeDtypeStruct(patches.shape, BF),
            jax.ShapeDtypeStruct((CHUNKS, PART, WIDE), F32),
            jax.ShapeDtypeStruct((32, 128), F32),
        ],
        in_specs=[smem] * 2 + [vmem] * 10 + [hbm] * 6,
        out_specs=[hbm, hbm, vmem, vmem],
        scratch_shapes=[
            packed(strips, row_count, width),
            packed(strips, row_count, width),
            wide(rows, width),
            packed(rows, width),
            packed(rows, 3 * width),
            packed(rows, width),
            wide(rows, 128),
            wide(rows, width),
            packed(rows, width),
            packed(rows, hidden_units),
            packed(rows, width),
            wide(rows, width),
            wide(rows, width),
            packed(rows, width),
            packed(rows, width),
            packed(rows, width),
            wide(width, width),
            wide(8, width),
            wide(16, width),
            packed(width, 3 * width),
            packed(width, width),
            packed(2, width, width),
            packed(2, width, width),
            packed(SLOTS, 2, 384, WIDE),
            packed(CHUNKS, 384, WIDE),
            packed(CHUNKS, 192, WIDE),
            packed(CHUNKS, 96, WIDE),
            packed(CHUNKS, 48, WIDE),
            wide(CHUNKS, 48, WIDE),
            wide(CHUNKS, 24, WIDE),
        ]
        + [wide(16, width)] * STAGES
        + [
            pltpu.SemaphoreType.DMA((STAGES, CHUNKS)),
            pltpu.SemaphoreType.DMA((STAGES, CHUNKS)),
            pltpu.SemaphoreType.DMA((STAGES,)),
            pltpu.SemaphoreType.DMA((STAGES,)),
            pltpu.SemaphoreType.DMA((4, strips)),
            pltpu.SemaphoreType.DMA((4, strips)),
            pltpu.SemaphoreType.DMA((2,)),
            pltpu.SemaphoreType.DMA((2, 2)),
            pltpu.SemaphoreType.DMA((4,)),
        ],
        compiler_params=pltpu.CompilerParams(
            collective_id=0, has_side_effects=True, vmem_limit_bytes=67043328
        ),
    )(*arrays)


def finish_kernel(
    layer_in, grad_in, reduced, small,
    layer_out, grad_patches, table, gain_one, bias_one, qkv, query_bias, value_bias, out_weight,
    out_bias, gain_two, bias_two, up_weight, up_bias, down_weight, down_bias,
):
    layer_out[...] = layer_in[...]
    grad_patches[...] = grad_in[...]
    names = (gain_one, bias_one, query_bias, value_bias, out_bias, gain_two, bias_two, down_bias)
    for index, ref in enumerate(names):
        ref[...] = small[pl.ds(index, 1), pl.ds(0, PART)].reshape(PART)
    up_bias[...] = column_sum(small[pl.ds(16, 16), pl.ds(0, 4 * PART)]).reshape(4 * PART)
    table[...] = small[pl.ds(8, 4), pl.ds(0, PART)].T
    for c in range(8):
        up_weight[:, pl.ds(c * WIDE, WIDE)] = reduced[c]
    for c in range(2):
        out_weight[:, pl.ds(c * WIDE, WIDE)] = reduced[8 + c]
    for half in range(2):
        for sub in range(4):
            down_weight[pl.ds(sub * PART, PART), pl.ds(half * WIDE, WIDE)] = reduced[
                10 + half * 4 + sub
            ]
    width = qkv.shape[1] // 3
    for pair in range(6):
        for part in range(3):
            qkv[:, pl.ds(part * width + pair * 128, 128)] = reduced[
                18 + pair, :, pl.ds(part * 128, 128)
            ]


def local(
    patches,
    lengths,
    script,
    script_table,
    gain_one,
    bias_one,
    qkv_weight,
    query_bias,
    value_bias,
    out_weight,
    out_bias,
    gain_two,
    bias_two,
    up_weight,
    up_bias,
    down_weight,
    down_bias,
    cotangent,
):
    strips, row_count, width = patches.shape
    groups = script_table.shape[0]
    results = run_layer(
        lengths, script, script_table, gain_one, bias_one, query_bias, value_bias, out_bias,
        gain_two, bias_two, up_bias.reshape(-1, width), down_bias, patches, cotangent, qkv_weight,
        out_weight, up_weight, down_weight,
    )
    vector = jax.ShapeDtypeStruct((PART,), F32)
    return pl.pallas_call(
        finish_kernel,
        out_shape=[
            jax.ShapeDtypeStruct(patches.shape, BF),
            jax.ShapeDtypeStruct(patches.shape, BF),
            jax.ShapeDtypeStruct((PART, groups), F32),
            vector,
            vector,
            jax.ShapeDtypeStruct((PART, 3 * width), F32),
            vector,
            vector,
            jax.ShapeDtypeStruct((PART, width), F32),
            vector,
            vector,
            vector,
            jax.ShapeDtypeStruct((PART, up_weight.shape[1]), F32),
            jax.ShapeDtypeStruct((4 * PART,), F32),
            jax.ShapeDtypeStruct((4 * PART, width), F32),
            vector,
        ],
    )(*results)


def solution(mesh):
    placed = (
        P("strip", "seq", None),
        P("strip"),
        P("strip"),
        P(),
        P(),
        P(),
        P(),
        P(),
        P(),
        P(),
        P(),
        P(),
        P(),
        P(),
        P(),
        P(),
        P(),
        P("strip", "seq", None),
    )
    chosen = local if fits(mesh) else local_general
    return jax.shard_map(
        chosen,
        mesh=mesh,
        in_specs=placed,
        out_specs=(
            P("strip", "seq", None),
            P("strip", "seq", None),
            P(("strip", "seq"), None),
            P(("strip", "seq")),
            P(("strip", "seq")),
            P(("strip", "seq"), None),
            P(("strip", "seq")),
            P(("strip", "seq")),
            P(("strip", "seq"), None),
            P(("strip", "seq")),
            P(("strip", "seq")),
            P(("strip", "seq")),
            P(("strip", "seq"), None),
            P(("strip", "seq")),
            P(("strip", "seq"), None),
            P(("strip", "seq")),
        ),
        check_vma=False,
    )
```

```python
import functools

import jax
import jax.numpy as jnp
from jax import lax
from jax.experimental import pallas as pl
from jax.experimental.pallas import tpu as pltpu
from jax.sharding import PartitionSpec as P

HD = 64


epsilon = 1e-12


def normalize(hidden):
    centred = hidden - jnp.mean(hidden, axis=-1, keepdims=True)
    inverse = lax.rsqrt(jnp.mean(centred * centred, axis=-1, keepdims=True) + epsilon)
    return (centred * inverse, inverse)


def norm_back(upstream, gain, normed, inverse):
    scaled = upstream * gain
    return inverse * (
        scaled
        - jnp.mean(scaled, axis=-1, keepdims=True)
        - normed * jnp.mean(scaled * normed, axis=-1, keepdims=True)
    )


def weight_grad(inputs, upstream):
    return lax.dot_general(
        inputs, upstream, (((0,), (0,)), ((), ())), preferred_element_type=jnp.float32
    )


def input_grad(upstream, weight):
    return lax.dot_general(
        upstream, weight, (((1,), (1,)), ((), ())), preferred_element_type=jnp.float32
    )


def gelu_slope(upper):
    return (
        0.5 * (1.0 + lax.erf(upper * 0.7071067811865476))
        + upper * jnp.exp(-0.5 * upper * upper) * 0.3989422804014327
    )


def split_block(block):
    seq_len = block.shape[0]
    heads_here = block.shape[2] // HD
    return [block[:, member].reshape(seq_len, heads_here, HD) for member in range(3)]


def masked_logits(queries, key_rows, length):
    logits = jnp.einsum(
        "qhd,khd->hqk", queries, key_rows, preferred_element_type=jnp.float32
    ) * HD ** (-0.5)
    visible = jnp.arange(logits.shape[-1], dtype=jnp.int32) < length
    return jnp.where(visible[None, None, :], logits, -1000000000.0)


def attend_forward(item):
    block, length = item
    queries, key_rows, values = split_block(block)
    logits = masked_logits(queries, key_rows, length)
    highest = jnp.max(logits, axis=-1, keepdims=True)
    expanded = jnp.exp(logits - highest)
    totals = jnp.sum(expanded, axis=-1, keepdims=True)
    probs = (expanded / totals).astype(jnp.bfloat16)
    mixed = jnp.einsum("hqk,khd->qhd", probs, values, preferred_element_type=jnp.float32)
    mixed = mixed.astype(jnp.bfloat16).reshape(block.shape[0], block.shape[2])
    return (mixed, (highest + jnp.log(totals))[..., 0])


def attend_backward(item):
    block, log_total, grad_mixed, length = item
    queries, key_rows, values = split_block(block)
    logits = masked_logits(queries, key_rows, length)
    probs = jnp.exp(logits - log_total[..., None])
    grad_heads = grad_mixed.reshape(queries.shape)
    grad_values = jnp.einsum(
        "hqk,qhd->khd", probs.astype(jnp.bfloat16), grad_heads, preferred_element_type=jnp.float32
    )
    grad_probs = jnp.einsum("qhd,khd->hqk", grad_heads, values, preferred_element_type=jnp.float32)
    inner = jnp.sum(probs * grad_probs, axis=-1, keepdims=True)
    grad_logits = (probs * (grad_probs - inner)).astype(jnp.bfloat16)
    grad_queries = jnp.einsum(
        "hqk,khd->qhd", grad_logits, key_rows, preferred_element_type=jnp.float32
    ) * HD ** (-0.5)
    grad_keys = jnp.einsum(
        "hqk,qhd->khd", grad_logits, queries, preferred_element_type=jnp.float32
    ) * HD ** (-0.5)
    stacked = jnp.stack([grad_queries, grad_keys, grad_values], axis=1)
    return stacked.reshape(block.shape).astype(jnp.bfloat16)


def local_general(
    patches,
    lengths,
    script,
    script_table,
    gain_one,
    bias_one,
    qkv_weight,
    query_bias,
    value_bias,
    out_weight,
    out_bias,
    gain_two,
    bias_two,
    up_weight,
    up_bias,
    down_weight,
    down_bias,
    cotangent,
):
    strips, row_count, model_width = patches.shape
    groups = script_table.shape[0]
    tokens = strips * row_count
    selector = (script[:, None] == jnp.arange(groups, dtype=jnp.int32)[None, :]).astype(jnp.float32)
    added = jnp.dot(selector.astype(jnp.bfloat16), script_table, preferred_element_type=jnp.float32)
    hidden = (patches.astype(jnp.float32) + added[:, None, :]).reshape(tokens, model_width)
    normed_one, inverse_one = normalize(hidden)
    inputs_one = (normed_one * gain_one + bias_one).astype(jnp.bfloat16)
    joint_bias = jnp.concatenate([query_bias, jnp.zeros_like(query_bias), value_bias])
    projected = (
        jnp.dot(inputs_one, qkv_weight, preferred_element_type=jnp.float32) + joint_bias
    ).astype(jnp.bfloat16)
    projected = projected.reshape(strips, row_count, 3, model_width)
    head_blocks = lax.all_to_all(projected, "seq", split_axis=3, concat_axis=1, tiled=True)
    mixed_heads, log_totals = lax.map(attend_forward, (head_blocks, lengths))
    mixed = lax.all_to_all(mixed_heads, "seq", split_axis=1, concat_axis=2, tiled=True).reshape(
        tokens, model_width
    )
    attended = hidden + jnp.dot(mixed, out_weight, preferred_element_type=jnp.float32) + out_bias
    normed_two, inverse_two = normalize(attended)
    inputs_two = (normed_two * gain_two + bias_two).astype(jnp.bfloat16)
    upper = jnp.dot(inputs_two, up_weight, preferred_element_type=jnp.float32) + up_bias
    active = jax.nn.gelu(upper, approximate=False).astype(jnp.bfloat16)
    result = attended + jnp.dot(active, down_weight, preferred_element_type=jnp.float32) + down_bias
    layer_out = result.astype(jnp.bfloat16).reshape(strips, row_count, model_width)
    grad_result = cotangent.reshape(tokens, model_width)
    grad_float = grad_result.astype(jnp.float32)
    grad_down_weight = weight_grad(active, grad_result)
    grad_down_bias = jnp.sum(grad_float, axis=0)
    grad_upper = (input_grad(grad_result, down_weight) * gelu_slope(upper)).astype(jnp.bfloat16)
    grad_up_weight = weight_grad(inputs_two, grad_upper)
    grad_up_bias = jnp.sum(grad_upper.astype(jnp.float32), axis=0)
    grad_inputs_two = input_grad(grad_upper, up_weight)
    grad_gain_two = jnp.sum(grad_inputs_two * normed_two, axis=0)
    grad_bias_two = jnp.sum(grad_inputs_two, axis=0)
    grad_attended = grad_float + norm_back(grad_inputs_two, gain_two, normed_two, inverse_two)
    grad_branch = grad_attended.astype(jnp.bfloat16)
    grad_out_weight = weight_grad(mixed, grad_branch)
    grad_out_bias = jnp.sum(grad_branch.astype(jnp.float32), axis=0)
    grad_mixed = (
        input_grad(grad_branch, out_weight)
        .astype(jnp.bfloat16)
        .reshape(strips, row_count, model_width)
    )
    grad_mixed_heads = lax.all_to_all(grad_mixed, "seq", split_axis=2, concat_axis=1, tiled=True)
    grad_heads = lax.map(attend_backward, (head_blocks, log_totals, grad_mixed_heads, lengths))
    grad_projected = lax.all_to_all(
        grad_heads, "seq", split_axis=1, concat_axis=3, tiled=True
    ).reshape(tokens, 3 * model_width)
    grad_qkv = weight_grad(inputs_one, grad_projected)
    grad_bias_rows = jnp.sum(grad_projected.astype(jnp.float32), axis=0)
    grad_query_bias = grad_bias_rows[:model_width]
    grad_value_bias = grad_bias_rows[2 * model_width :]
    grad_inputs_one = input_grad(grad_projected, qkv_weight)
    grad_gain_one = jnp.sum(grad_inputs_one * normed_one, axis=0)
    grad_bias_one = jnp.sum(grad_inputs_one, axis=0)
    grad_hidden = grad_attended + norm_back(grad_inputs_one, gain_one, normed_one, inverse_one)
    grad_patches = grad_hidden.astype(jnp.bfloat16).reshape(strips, row_count, model_width)
    per_strip = jnp.sum(grad_hidden.reshape(strips, row_count, model_width), axis=1)
    grad_table = jnp.dot(per_strip.T, selector, precision=lax.Precision.HIGHEST)
    summed = (
        lax.psum_scatter(grad_table, ("strip", "seq"), scatter_dimension=0, tiled=True),
        lax.psum_scatter(grad_gain_one, ("strip", "seq"), scatter_dimension=0, tiled=True),
        lax.psum_scatter(grad_bias_one, ("strip", "seq"), scatter_dimension=0, tiled=True),
        lax.psum_scatter(grad_qkv, ("strip", "seq"), scatter_dimension=0, tiled=True),
        lax.psum_scatter(grad_query_bias, ("strip", "seq"), scatter_dimension=0, tiled=True),
        lax.psum_scatter(grad_value_bias, ("strip", "seq"), scatter_dimension=0, tiled=True),
        lax.psum_scatter(grad_out_weight, ("strip", "seq"), scatter_dimension=0, tiled=True),
        lax.psum_scatter(grad_out_bias, ("strip", "seq"), scatter_dimension=0, tiled=True),
        lax.psum_scatter(grad_gain_two, ("strip", "seq"), scatter_dimension=0, tiled=True),
        lax.psum_scatter(grad_bias_two, ("strip", "seq"), scatter_dimension=0, tiled=True),
        lax.psum_scatter(grad_up_weight, ("strip", "seq"), scatter_dimension=0, tiled=True),
        lax.psum_scatter(grad_up_bias, ("strip", "seq"), scatter_dimension=0, tiled=True),
        lax.psum_scatter(grad_down_weight, ("strip", "seq"), scatter_dimension=0, tiled=True),
        lax.psum_scatter(grad_down_bias, ("strip", "seq"), scatter_dimension=0, tiled=True),
    )
    return (
        layer_out,
        grad_patches,
        summed[0],
        summed[1],
        summed[2],
        summed[3],
        summed[4],
        summed[5],
        summed[6],
        summed[7],
        summed[8],
        summed[9],
        summed[10],
        summed[11],
        summed[12],
        summed[13],
    )


MESH = pl.DeviceIdType.MESH
BF = jnp.bfloat16
F32 = jnp.float32
CHUNKS = 24
OWN = 16
SLOTS = 4
STAGES = 5
WIDE = 384
PART = 24
BLOCK = 32

PLAN = {
    "ffn": [
        [
            (0, 0, 0, 0, 0, 0, 0, 0, 0, 0, 0, 0, 0, 0, 0, 0, 0, 0, 0, 0),
            (0, 0, 0, 0, 0, 0, 0, 0, 0, 0, 2, 0, 0, 0, 0, 2, 0, 0, 0, 0),
            (2, 0, 0, 0, 0, 2, 0, 0, 0, 0, 4, 0, 0, 0, 0, 4, 0, 0, 0, 0),
            (4, 2, 0, 0, 0, 4, 1, 0, 0, 0, 6, 4, 0, 0, 0, 6, 3, 0, 0, 0),
        ],
        [
            (0, 0, 0, 0, 0, 0, 0, 0, 0, 0, 0, 0, 0, 0, 0, 0, 0, 0, 0, 0),
            (2, 0, 0, 0, 0, 2, 0, 0, 0, 0, 2, 0, 0, 0, 0, 2, 0, 0, 0, 0),
            (4, 0, 0, 0, 0, 4, 0, 0, 0, 0, 4, 2, 0, 0, 0, 4, 1, 0, 0, 0),
            (6, 4, 0, 0, 0, 6, 3, 0, 0, 0, 6, 4, 1, 0, 0, 6, 3, 0, 0, 0),
        ],
        [
            (0, 0, 0, 0, 0, 0, 0, 0, 0, 0, 0, 0, 0, 0, 0, 0, 0, 0, 0, 0),
            (2, 0, 0, 0, 0, 2, 0, 0, 0, 0, 2, 0, 0, 0, 0, 2, 0, 0, 0, 0),
            (4, 2, 0, 0, 0, 4, 1, 0, 0, 0, 4, 2, 0, 0, 0, 4, 1, 0, 0, 0),
            (6, 4, 1, 0, 0, 6, 3, 0, 0, 0, 6, 4, 1, 0, 0, 6, 4, 0, 0, 0),
        ],
    ],
    "after": [
        (6, 4, 1, 0, 0, 6, 4, 0, 0, 0, 8, 4, 3, 0, 0, 8, 4, 0, 0, 0),
        (8, 4, 3, 0, 0, 8, 4, 0, 0, 0, 8, 4, 3, 0, 0, 8, 4, 2, 0, 0),
        (8, 4, 3, 0, 0, 8, 4, 2, 0, 0, 8, 4, 4, 1, 0, 8, 4, 2, 0, 0),
    ],
    "pair": [
        (8, 4, 4, 1, 0, 8, 4, 2, 0, 0, 10, 4, 4, 1, 0, 8, 5, 3, 0, 0),
        (10, 4, 4, 1, 0, 8, 5, 3, 0, 0, 10, 6, 4, 1, 0, 8, 5, 3, 0, 0),
        (10, 6, 4, 1, 1, 8, 6, 3, 3, 0, 12, 8, 4, 1, 1, 8, 6, 3, 3, 0),
        (12, 8, 4, 1, 1, 8, 6, 3, 3, 0, 12, 8, 4, 3, 1, 8, 6, 5, 3, 2),
        (12, 10, 4, 4, 1, 8, 8, 5, 3, 3, 14, 10, 8, 4, 3, 8, 8, 6, 4, 3),
        (14, 10, 8, 4, 3, 8, 8, 6, 4, 3, 14, 12, 9, 4, 4, 8, 8, 6, 5, 3),
    ],
    "grad": [
        [
            (10, 6, 4, 1, 0, 8, 5, 3, 0, 0, 10, 6, 4, 1, 0, 8, 6, 3, 2, 0),
            (12, 8, 4, 3, 1, 8, 6, 5, 3, 2, 12, 8, 4, 4, 1, 8, 8, 5, 3, 3),
            (14, 12, 9, 4, 4, 8, 8, 6, 5, 3, 14, 12, 9, 6, 4, 8, 8, 8, 5, 3),
        ],
        [
            (10, 6, 4, 1, 0, 8, 6, 3, 2, 0, 10, 6, 4, 1, 1, 8, 6, 3, 3, 0),
            (12, 8, 4, 4, 1, 8, 8, 5, 3, 3, 12, 10, 4, 4, 1, 8, 8, 5, 3, 3),
            (14, 12, 9, 6, 4, 8, 8, 8, 5, 3, 14, 12, 10, 8, 4, 8, 8, 8, 5, 4),
        ],
    ],
    "last": [
        (14, 12, 10, 8, 4, 8, 8, 8, 5, 4, 16, 13, 11, 8, 4, 8, 8, 8, 6, 4),
        (16, 13, 11, 8, 4, 8, 8, 8, 6, 4, 16, 14, 11, 8, 4, 8, 8, 8, 6, 4),
    ],
    "tail": [
        (16, 14, 11, 8, 4, 8, 8, 8, 6, 4, 16, 14, 12, 8, 4, 8, 8, 8, 6, 4),
        (16, 14, 12, 8, 4, 8, 8, 8, 6, 4, 16, 14, 12, 10, 4, 8, 8, 8, 6, 4),
        (16, 14, 12, 10, 4, 8, 8, 8, 6, 4, 16, 14, 12, 10, 4, 8, 8, 8, 6, 5),
        (16, 14, 12, 10, 4, 8, 8, 8, 6, 5, 16, 14, 12, 10, 5, 8, 8, 8, 6, 5),
        (16, 14, 12, 10, 5, 8, 8, 8, 6, 5, 16, 14, 12, 10, 6, 8, 8, 8, 6, 5),
        (16, 14, 12, 10, 6, 8, 8, 8, 6, 5, 16, 14, 12, 10, 6, 8, 8, 8, 7, 5),
        (16, 14, 12, 10, 6, 8, 8, 8, 7, 5, 16, 14, 13, 10, 6, 8, 8, 8, 7, 5),
        (16, 14, 13, 10, 6, 8, 8, 8, 7, 5, 16, 14, 13, 10, 6, 8, 8, 8, 8, 5),
        (16, 14, 13, 10, 6, 8, 8, 8, 8, 5, 16, 14, 13, 10, 7, 8, 8, 8, 8, 5),
        (16, 14, 13, 10, 7, 8, 8, 8, 8, 5, 16, 14, 13, 10, 8, 8, 8, 8, 8, 5),
        (16, 14, 13, 10, 8, 8, 8, 8, 8, 5, 16, 15, 13, 10, 8, 8, 8, 8, 8, 5),
        (16, 15, 13, 10, 8, 8, 8, 8, 8, 5, 16, 15, 13, 11, 8, 8, 8, 8, 8, 5),
        (16, 15, 13, 11, 8, 8, 8, 8, 8, 5, 16, 15, 13, 11, 8, 8, 8, 8, 8, 6),
        (16, 15, 13, 11, 8, 8, 8, 8, 8, 6, 16, 15, 14, 11, 8, 8, 8, 8, 8, 6),
        (16, 15, 14, 11, 8, 8, 8, 8, 8, 6, 16, 16, 14, 11, 8, 8, 8, 8, 8, 6),
        (16, 16, 14, 11, 8, 8, 8, 8, 8, 6, 16, 16, 14, 11, 9, 8, 8, 8, 8, 6),
        (16, 16, 14, 11, 9, 8, 8, 8, 8, 6, 16, 16, 14, 11, 10, 8, 8, 8, 8, 6),
        (16, 16, 14, 11, 10, 8, 8, 8, 8, 6, 16, 16, 14, 13, 10, 8, 8, 8, 8, 6),
        (16, 16, 14, 13, 10, 8, 8, 8, 8, 6, 16, 16, 14, 13, 10, 8, 8, 8, 8, 7),
        (16, 16, 14, 13, 10, 8, 8, 8, 8, 7, 16, 16, 15, 13, 10, 8, 8, 8, 8, 7),
        (16, 16, 15, 13, 10, 8, 8, 8, 8, 7, 16, 16, 15, 14, 11, 8, 8, 8, 8, 7),
        (16, 16, 15, 14, 11, 8, 8, 8, 8, 7, 16, 16, 16, 14, 11, 8, 8, 8, 8, 8),
        (16, 16, 16, 14, 11, 8, 8, 8, 8, 8, 16, 16, 16, 14, 12, 8, 8, 8, 8, 8),
        (16, 16, 16, 14, 12, 8, 8, 8, 8, 8, 16, 16, 16, 14, 13, 8, 8, 8, 8, 8),
        (16, 16, 16, 14, 13, 8, 8, 8, 8, 8, 16, 16, 16, 15, 13, 8, 8, 8, 8, 8),
        (16, 16, 16, 15, 13, 8, 8, 8, 8, 8, 16, 16, 16, 16, 13, 8, 8, 8, 8, 8),
        (16, 16, 16, 16, 13, 8, 8, 8, 8, 8, 16, 16, 16, 16, 14, 8, 8, 8, 8, 8),
        (16, 16, 16, 16, 14, 8, 8, 8, 8, 8, 16, 16, 16, 16, 15, 8, 8, 8, 8, 8),
        (16, 16, 16, 16, 15, 8, 8, 8, 8, 8, 16, 16, 16, 16, 16, 8, 8, 8, 8, 8),
    ],
}


def fits(mesh):
    return dict(mesh.shape) == {"strip": 8, "seq": 4}


def dot(left, right, left_dim, right_dim):
    return lax.dot_general(
        left, right, (((left_dim,), (right_dim,)), ((), ())), preferred_element_type=F32
    )


def mean(block):
    return jnp.mean(block, axis=1, keepdims=True)


def fold(block):
    return jnp.sum(block.reshape(block.shape[0] // 8, 8, block.shape[1]), axis=0)


def sweep(blocks, body, totals):
    def trip(first, size, totals):
        results = [body(first + k) for k in range(size)]
        for stores, _ in results:
            for ref, at, value in stores:
                ref[at] = value
        return tuple(
            total + sum(sums[k] for _, sums in results) for k, total in enumerate(totals)
        )

    totals = lax.fori_loop(0, blocks // 4, lambda i, t: trip(4 * i, 4, t), totals)
    if blocks % 4:
        totals = trip(blocks // 4 * 4, blocks % 4, totals)
    return totals


def block_rows(b):
    if isinstance(b, int):
        return pl.ds(b * BLOCK, BLOCK)
    return pl.ds(pl.multiple_of(b * BLOCK, BLOCK), BLOCK)


def column_sum(block):
    return jnp.sum(block, axis=0, keepdims=True)


def attend_pair(pair, length, proj, mixed, lse_all):
    count = proj.shape[0]
    width = proj.shape[1] // 3
    at = lambda part: pl.ds(pl.multiple_of(part * width + pair * 128, 128), 128)
    lane = lax.broadcasted_iota(jnp.int32, (1, 128), 1)
    visible = lax.broadcasted_iota(jnp.int32, (1, count), 1) < length
    q = proj[:, at(0)] * jnp.asarray(0.125, BF)
    k = proj[:, at(1)]
    v = proj[:, at(2)]
    outs, logs = [], []
    for head in range(2):
        own = (lane // HD) == head
        logits = dot(jnp.where(own, q, jnp.zeros_like(q)), k, 1, 1)
        logits = jnp.where(visible, logits, -1000000000.0)
        highest = jnp.max(logits, axis=1, keepdims=True)
        expanded = jnp.exp(logits - highest)
        total = jnp.sum(expanded, axis=1, keepdims=True)
        probs = (expanded * (1.0 / total)).astype(BF)
        outs.append(dot(probs, v, 1, 0))
        logs.append(highest + jnp.log(total))
    mixed[:, at(0)] = jnp.where(lane < HD, outs[0], outs[1]).astype(BF)
    known = jnp.where(lane == 2 * pair, logs[0], lse_all[...])
    lse_all[...] = jnp.where(lane == 2 * pair + 1, logs[1], known)


def attend_pair_back(pair, length, proj, gmixed, lse_all):
    count = proj.shape[0]
    width = proj.shape[1] // 3
    at = lambda part: pl.ds(pl.multiple_of(part * width + pair * 128, 128), 128)
    lane = lax.broadcasted_iota(jnp.int32, (1, 128), 1)
    visible = lax.broadcasted_iota(jnp.int32, (1, count), 1) < length
    q = proj[:, at(0)] * jnp.asarray(0.125, BF)
    k = proj[:, at(1)]
    v = proj[:, at(2)]
    gm = gmixed[:, at(0)]
    lse = lse_all[...]
    grads = []
    for head in range(2):
        own = (lane // HD) == head
        q_own = jnp.where(own, q, jnp.zeros_like(q))
        g_own = jnp.where(own, gm, jnp.zeros_like(gm))
        k_own = jnp.where(own, k, jnp.zeros_like(k))
        own_lse = jnp.sum(jnp.where(lane == 2 * pair + head, lse, 0.0), axis=1, keepdims=True)
        logits = dot(q_own, k, 1, 1)
        probs = jnp.where(visible, jnp.exp(logits - own_lse), 0.0)
        grad_probs = dot(g_own, v, 1, 1)
        inner = jnp.sum(probs * grad_probs, axis=1, keepdims=True)
        grad_logits = (probs * (grad_probs - inner)).astype(BF)
        grads.append(
            (
                dot(grad_logits, k_own, 1, 0),
                dot(q_own, grad_logits, 0, 0),
                dot(g_own, probs.astype(BF), 0, 0),
            )
        )
    gq = ((grads[0][0] + grads[1][0]) * 0.125).astype(BF)
    gk = (grads[0][1] + grads[1][1]).T.astype(BF)
    gv = (grads[0][2] + grads[1][2]).T.astype(BF)
    return gq, gk, gv


class Devices:
    def __init__(self):
        s, q = lax.axis_index("strip"), lax.axis_index("seq")
        self.s, self.q = s, q
        self.core, self.y = q % 2, q // 2
        self.x, self.low, self.high = s % 2, (s // 2) % 2, s // 4
        self.to_core = (s, q + 1 - 2 * self.core)
        self.to_y = (s, q + 2 - 4 * self.y)
        self.to_x = (s + 1 - 2 * self.x, q)
        self.to_low = (s + 2 - 4 * self.low, q)
        self.to_high = (s + 4 - 8 * self.high, q)
        self.to_far = (s + 2 - 4 * self.low + 4 - 8 * self.high, q)


def pick(index, values):
    chosen = values[0]
    for position in range(1, len(values)):
        change = values[position] - values[position - 1]
        if change:
            chosen = chosen + jnp.where(index >= position, change, 0)
    return chosen


class Reduction:
    def __init__(self, dev, g, r1, r2, r3, r4, s4, r5, r4d, r5d, write, write_down, send, recv):
        self.dev = dev
        self.bufs = (g, r1, r2, r3, r4, s4, r5, r4d, r5d)
        self.write = write
        self.write_down = write_down
        self.sems = (send, recv)

    def side(self, stage, c, down):
        dev = self.dev
        odd = c % 2
        even = 1 - odd
        if down:
            by_x, by_y, by_low = ((odd, even, 0), (even, odd, 0), (0, 0, 1))[stage - 1]
        else:
            by_x, by_y, by_low = ((even, 0, odd), (odd, even, 0), (0, odd, even))[stage - 1]
        device = (
            dev.s + by_x * (1 - 2 * dev.x) + by_low * (2 - 4 * dev.low),
            dev.q + by_y * (2 - 4 * dev.y),
        )
        return device, by_x * dev.x + by_y * dev.y + by_low * dev.low

    def slot(self, c, down):
        return c % SLOTS + SLOTS if down else c % SLOTS

    def copy(self, stage, c, down):
        g, r1, r2, r3, r4, s4, r5, r4d, r5d = self.bufs
        dev = self.dev
        if stage == 0:
            source, target = g.at[self.slot(c, down), 1 - dev.core], r1.at[c]
            device = dev.to_core
        elif stage == 4:
            device = dev.to_high
            if down:
                source, target = r4d.at[c - OWN], r5d.at[c - OWN]
            else:
                source, target = s4.at[c, 1 - dev.high], r5.at[c]
        elif stage == 3 and down:
            source, target, device = r3.at[c], r4d.at[c - OWN], dev.to_low
        else:
            device, bit = self.side(stage, c, down)
            rows = 384 >> stage
            held, target = ((r1, r2), (r2, r3), (r3, r4))[stage - 1]
            source, target = held.at[c, pl.ds((1 - bit) * rows, rows)], target.at[c]
        send, recv = self.sems
        return pltpu.make_async_remote_copy(
            src_ref=source,
            dst_ref=target,
            send_sem=send.at[stage, c],
            recv_sem=recv.at[stage, c],
            device_id=device,
            device_id_type=MESH,
        )

    def near(self, c):
        return self.dev.low == (c - OWN) // 2 % 2

    def far(self, c):
        return self.dev.high == (c - OWN) // 4

    def free(self, c, down):
        first = OWN if down else 0

        @pl.when(c >= first + SLOTS)
        def _():
            self.copy(0, c - SLOTS, down).wait_send()

    def start(self, c, down):
        self.copy(0, c, down).start()

    def event(self, stage, c, down):
        g, r1, r2, r3, r4, s4, r5, r4d, r5d = self.bufs
        dev = self.dev
        if stage >= 3 and down:
            self.last_events(stage, c)
            return
        self.copy(stage, c, down).wait_recv()
        if stage == 0:
            slot = self.slot(c, down)

            @pl.loop(0, 4)
            def _(i):
                rows = pl.ds(i * 96, 96)
                r1[c, rows] = r1[c, rows] + g[slot, dev.core, rows]
        elif stage < 3:
            _, bit = self.side(stage, c, down)
            held, target = ((r1, r2), (r2, r3))[stage - 1]

            @pl.loop(0, 4 >> stage)
            def _(i):
                rows = pl.ds(i * 96, 96)
                kept = pl.ds(pl.multiple_of(bit * (384 >> stage) + i * 96, 96), 96)
                target[c, rows] = target[c, rows] + held[c, kept]
        elif stage == 3:
            _, bit = self.side(stage, c, down)
            kept = pl.ds(pl.multiple_of(bit * 48, 48), 48)
            total = r4[c].astype(F32) + r3[c, kept].astype(F32)
            s4[c, 0] = total[:24].astype(BF)
            s4[c, 1] = total[24:].astype(BF)
        else:
            self.write[c] = s4[c, dev.high].astype(F32) + r5[c].astype(F32)
            return
        if stage == 2 and down:

            @pl.when(jnp.logical_not(self.near(c)))
            def _():
                self.copy(3, c, down).start()
        else:
            self.copy(stage + 1, c, down).start()

    def last_events(self, stage, c):
        r3, r4d, r5d = self.bufs[3], self.bufs[7], self.bufs[8]

        @pl.when(self.near(c))
        def _():
            if stage == 3:
                self.copy(3, c, True).wait_recv()
                r4d[c - OWN] = r4d[c - OWN] + r3[c]

                @pl.when(jnp.logical_not(self.far(c)))
                def _():
                    self.copy(4, c, True).start()
            else:

                @pl.when(self.far(c))
                def _():
                    self.copy(4, c, True).wait_recv()
                    total = r4d[c - OWN].astype(F32) + r5d[c - OWN].astype(F32)
                    self.write_down[c % 2] = total

    def step(self, plans, index=0):
        for column in (4, 9, 3, 8, 2, 7, 1, 6, 0, 5):
            low = pick(index, [plan[column] for plan in plans])
            high = pick(index, [plan[2 * STAGES + column] for plan in plans])
            if all(plan[column] == plan[2 * STAGES + column] for plan in plans):
                continue
            down = column >= STAGES
            first = OWN if down else 0

            @pl.loop(low + first, high + first)
            def _(c):
                self.event(column % STAGES, c, down)

    def finish(self):
        for down in (False, True):
            first, last = (OWN, CHUNKS) if down else (0, OWN)

            @pl.loop(last - SLOTS, last)
            def _(c):
                self.copy(0, c, down).wait_send()

            @pl.loop(first, last)
            def _(c):
                for stage in range(1, STAGES):
                    if down and stage == 3:

                        @pl.when(jnp.logical_not(self.near(c)))
                        def _():
                            self.copy(3, c, True).wait_send()
                    elif down and stage == 4:

                        @pl.when(self.near(c) & jnp.logical_not(self.far(c)))
                        def _():
                            self.copy(4, c, True).wait_send()
                    else:
                        self.copy(stage, c, down).wait_send()

    def place(self, c, half, product):
        columns = pl.ds(half * WIDE, WIDE)
        for owner in range(32):
            core, y, x, low, high = [(owner >> bit) % 2 for bit in range(5)]
            unit = 4 * low + 2 * x + y if half else 4 * x + 2 * y + low
            self.bufs[0][self.slot(c, False), core, pl.ds(unit * 48 + high * PART, PART)] = product[
                pl.ds(owner * PART, PART), columns
            ]

    def place_down(self, c, half, product):
        columns = pl.ds(half * WIDE, WIDE)
        for owner in range(8):
            core, y, x = [(owner >> bit) % 2 for bit in range(3)]
            unit = 2 * x + y if half else 2 * y + x
            self.bufs[0][self.slot(c, True), core, pl.ds(unit * 96, 96)] = product[
                pl.ds(owner * 96, 96), columns
            ]


ERF_TOP = (
    0.00022905065861350646, 0.0034082910107109506, 0.050955695062380861, 0.18520832239976145,
    1.128379143519084,
)
ERF_BOTTOM = (
    -1.1791602954361697e-7, 0.000023547966471313185, 0.0010179625278914885,
    0.014070470171167667, 0.11098505178285362, 0.49746925110067538, 1.0,
)


def erf(value):
    value = jnp.clip(value, -3.832506856900711, 3.832506856900711)
    square = value * value
    top = jnp.full_like(square, ERF_TOP[0])
    for term in ERF_TOP[1:]:
        top = top * square + term
    bottom = jnp.full_like(square, ERF_BOTTOM[0])
    for term in ERF_BOTTOM[1:]:
        bottom = bottom * square + term
    return value * top / bottom


def standardize(block):
    centred = block - mean(block)
    inverse = lax.rsqrt(mean(centred * centred) + epsilon)
    return centred * inverse, inverse


def layer_kernel(
    lengths, script, table, gain_one, bias_one, query_bias, value_bias, out_bias, gain_two,
    bias_two, up_bias, down_bias, patches, cotangent, qkv_hbm, out_hbm, up_hbm, down_hbm,
    layer_out, grad_patches, reduced, reduced_down, small,
    outgoing, xin, cin, hidden, n1, proj, mixed, lse_all, att, n2, cot, res, gn, branch, gmixed,
    gblk, act, product, jbias, ubias, early, late, wqkv, wout, wup, wdown,
    g, r1, r2, r3, r4, s4, r5, r4d, r5d, early_in, late_in,
    send, recv, vsend, vrecv, xsend, xrecv, wsem, fsem, osem,
):
    row_count, strips, width = patches.shape
    count = strips * row_count
    rows = hidden.shape[0]
    blocks = rows // BLOCK
    ff_blocks = up_hbm.shape[1] // width
    dev = Devices()
    s, q = dev.s, dev.q
    red = Reduction(
        dev, g, r1, r2, r3, r4, s4, r5, r4d, r5d, reduced, reduced_down, send, recv
    )

    barrier = pltpu.get_barrier_semaphore()
    greeted = [(s, (q + hop) % strips) for hop in range(1, strips)]
    greeted += [dev.to_x, dev.to_low, dev.to_high, dev.to_far]
    for device in greeted:
        pl.semaphore_signal(barrier, inc=1, device_id=device, device_id_type=MESH)

    load_qkv = pltpu.make_async_copy(qkv_hbm, wqkv, wsem.at[0])
    load_out = pltpu.make_async_copy(out_hbm, wout, wsem.at[1])

    def load_ff(block):
        columns = pl.ds(pl.multiple_of(block * width, width), width)
        slot = block % 2
        return (
            pltpu.make_async_copy(up_hbm.at[:, columns], wup.at[slot], fsem.at[0, slot]),
            pltpu.make_async_copy(down_hbm.at[columns], wdown.at[slot], fsem.at[1, slot]),
        )

    def exchange(group, source, target):
        copies = []
        for hop in range(1, strips):
            other = (q + hop) % strips
            copies.append(
                pltpu.make_async_remote_copy(
                    src_ref=source.at[other],
                    dst_ref=target.at[q],
                    send_sem=xsend.at[group, hop],
                    recv_sem=xrecv.at[group, hop],
                    device_id=(s, other),
                    device_id_type=MESH,
                )
            )
        own = pltpu.make_async_copy(source.at[q], target.at[q], osem.at[group])
        return copies, own

    def launch(moves):
        copies, own = moves
        for index in (1, 0, 2):
            copies[index].start()
        own.start()

    def arrive(moves):
        copies, own = moves
        for copy in copies:
            copy.wait_recv()
        own.wait()

    def share(group, total, arrived):
        steps = [
            [(s, (q + hop) % strips) for hop in range(1, strips)],
            [dev.to_x],
            [dev.to_low, dev.to_high, dev.to_far],
        ]

        def copies(step):
            first = (0, 3, 4)[step]
            return [
                pltpu.make_async_remote_copy(
                    src_ref=total,
                    dst_ref=arrived.at[first + k],
                    send_sem=vsend.at[group, first + k],
                    recv_sem=vrecv.at[group, first + k],
                    device_id=device,
                    device_id_type=MESH,
                )
                for k, device in enumerate(steps[step])
            ]

        def begin(step):
            for copy in copies(step):
                copy.start()

        def end(step):
            first = (0, 3, 4)[step]
            moves = copies(step)
            for copy in moves:
                copy.wait_recv()
            for copy in moves:
                copy.wait_send()
            total[...] = total[...] + sum(arrived[first + k] for k in range(len(moves)))
            if step < 2:
                begin(step + 1)

        return begin, end

    def sent(moves):
        for copy in moves[0]:
            copy.wait_send()
        return moves

    into_x = exchange(0, outgoing, xin)
    into_c = exchange(1, outgoing, cin)
    for j in range(strips):
        outgoing[j] = patches[:, j, :]
    pl.semaphore_wait(barrier, len(greeted))
    launch(into_x)
    load_qkv.start()
    load_out.start()
    for copy in load_ff(0):
        copy.start()

    length = lengths[q]
    own_script = script[q]
    added = jnp.zeros((1, width), F32)
    for group in range(table.shape[0]):
        added = jnp.where(own_script == group, table[pl.ds(group, 1)].astype(F32), added)
    row = lambda ref: ref[...].reshape(1, ref.shape[0])
    jbias[pl.ds(0, 1)] = row(query_bias)
    jbias[pl.ds(1, 1)] = jnp.zeros((1, width), F32)
    jbias[pl.ds(2, 1)] = row(value_bias)
    hidden[pl.ds(count, rows - count)] = jnp.zeros((rows - count, width), F32)
    gn[pl.ds(count, rows - count)] = jnp.zeros((rows - count, width), F32)
    lse_all[...] = jnp.zeros_like(lse_all)

    for block in range(ff_blocks):
        ubias[pl.ds(block, 1)] = row(up_bias)[:, block * width : block * width + width]

    arrive(into_x)
    sent(into_x)
    for j in range(strips):
        outgoing[j] = cotangent[:, j, :]
    launch(into_c)
    for j in range(strips):
        hidden[pl.ds(j * row_count, row_count)] = xin[j].astype(F32) + added

    def first_norm(b):
        at = block_rows(b)
        normed, _ = standardize(hidden[at])
        return [(n1, at, (normed * row(gain_one) + row(bias_one)).astype(BF))], ()

    sweep(blocks, first_norm, ())

    load_qkv.wait()

    @pl.loop(0, 3)
    def _(part):
        columns = pl.ds(pl.multiple_of(part * width, width), width)
        proj[:, columns] = (dot(n1[...], wqkv[:, columns], 1, 0) + jbias[pl.ds(part, 1)]).astype(BF)

    @pl.loop(0, width // 128)
    def _(pair):
        attend_pair(pair, length, proj, mixed, lse_all)

    arrive(into_c)
    for j in range(strips):
        gn[pl.ds(j * row_count, row_count)] = cin[j].astype(F32)
    load_out.wait()
    att[...] = hidden[...] + dot(mixed[...], wout[...], 1, 0) + row(out_bias)
    zero8 = jnp.zeros((8, width), F32)

    def second_norm(b):
        at = block_rows(b)
        block = att[at]
        normed, _ = standardize(block)
        upstream = gn[at]
        stores = [
            (n2, at, (normed * row(gain_two) + row(bias_two)).astype(BF)),
            (res, at, block + row(down_bias)),
            (cot, at, upstream.astype(BF)),
            (gn, at, jnp.zeros((BLOCK, width), F32)),
        ]
        return stores, (fold(upstream),)

    early[pl.ds(3, 1)] = column_sum(sweep(blocks, second_norm, (zero8,))[0])

    @pl.loop(0, ff_blocks)
    def _(block):
        slot = block % 2
        for copy in load_ff(block):
            copy.wait()

        @pl.when(block + 1 < ff_blocks)
        def _():
            for copy in load_ff(block + 1):
                copy.start()

        up = wup[slot]
        down = wdown[slot]
        upper = dot(n2[...], up, 1, 0) + ubias[pl.ds(block, 1)]
        grad_active = dot(cot[...], down, 1, 1)
        share = 0.5 * (1.0 + erf(upper * 0.7071067811865476))
        act[...] = (upper * share).astype(BF)
        slope = share + upper * jnp.exp(-0.5 * upper * upper) * 0.3989422804014327
        grad_upper = (grad_active * slope).astype(BF)
        gblk[...] = grad_upper
        res[...] += dot(act[...], down, 1, 0)
        gn[...] += dot(grad_upper, up, 1, 1)
        early[pl.ds(4 + block, 1)] = column_sum(grad_upper.astype(F32))
        red.step(PLAN["ffn"][0], block)
        product[...] = dot(n2[...], gblk[...], 0, 0).astype(BF)
        for half in range(2):
            c = 2 * block + half
            red.free(c, False)
            red.place(c, half, product)
            red.start(c, False)
        red.step(PLAN["ffn"][1], block)
        product[...] = dot(act[...], cot[...], 0, 0).astype(BF)
        for half in range(2):
            c = OWN + 2 * block + half
            red.free(c, True)
            red.place_down(c, half, product)
            red.start(c, True)
        red.step(PLAN["ffn"][2], block)

    sent(into_c)
    for j in range(strips):
        outgoing[j] = res[pl.ds(j * row_count, row_count)].astype(BF)
    from_out = exchange(2, outgoing, layer_out)
    launch(from_out)

    def second_back(b):
        at = block_rows(b)
        normed, inverse = standardize(att[at])
        upstream = gn[at]
        scaled = upstream * row(gain_two)
        back = inverse * (scaled - mean(scaled) - normed * mean(scaled * normed))
        grad = cot[at].astype(F32) + back
        rounded = grad.astype(BF)
        sums = (fold(upstream * normed), fold(upstream), fold(rounded.astype(F32)))
        return [(gn, at, grad), (branch, at, rounded)], sums

    totals = sweep(blocks, second_back, (zero8, zero8, zero8))
    early[pl.ds(0, 1)] = column_sum(totals[0])
    early[pl.ds(1, 1)] = column_sum(totals[1])
    early[pl.ds(2, 1)] = column_sum(totals[2])
    share_early = share(0, early, early_in)
    share_early[0](0)
    red.step(PLAN["after"][:1])
    gmixed[...] = dot(branch[...], wout[...], 1, 1).astype(BF)
    red.step(PLAN["after"][1:2])
    product[...] = dot(mixed[...], branch[...], 0, 0).astype(BF)
    for half in range(2):
        c = 8 + half
        red.free(c, False)
        red.place(c, half, product)
        red.start(c, False)
    red.step(PLAN["after"][2:])

    res[...] = jnp.zeros_like(res)

    @pl.loop(0, 3)
    def _(i):
        @pl.loop(0, 2)
        def _(h):
            pair = 2 * i + h
            grads = attend_pair_back(pair, length, proj, gmixed, lse_all)
            for part in range(3):
                gblk[:, pl.ds(pl.multiple_of(h * WIDE + part * 128, 128), 128)] = grads[part]
            lanes = pl.ds(pl.multiple_of(pair * 128, 128), 128)
            late[pl.ds(2, 1), lanes] = column_sum(grads[0].astype(F32))
            late[pl.ds(3, 1), lanes] = column_sum(grads[2].astype(F32))
            red.step(PLAN["pair"], pair)

        product[...] = dot(n1[...], gblk[...], 0, 0).astype(BF)
        for half in range(2):
            c = 10 + 2 * i + half
            red.free(c, False)
            red.place(c, half, product)
            red.start(c, False)
        red.step(PLAN["grad"][0], i)
        weights = jnp.concatenate(
            [
                wqkv[:, pl.ds(pl.multiple_of(part * width + (2 * i + h) * 128, 128), 128)]
                for h in range(2)
                for part in range(3)
            ],
            axis=1,
        )
        res[...] += dot(gblk[...], weights, 1, 1)
        red.step(PLAN["grad"][1], i)
        for turn in range(3):

            @pl.when(i == turn)
            def _():
                share_early[1](turn)

    def first_back(b):
        at = block_rows(b)
        normed, inverse = standardize(hidden[at])
        upstream = res[at]
        scaled = upstream * row(gain_one)
        back = inverse * (scaled - mean(scaled) - normed * mean(scaled * normed))
        grad = gn[at] + back
        return [(res, at, grad)], (fold(upstream * normed), fold(upstream), fold(grad))

    totals = sweep(blocks, first_back, (zero8, zero8, zero8))
    red.step(PLAN["last"][:1])
    late[pl.ds(0, 1)] = column_sum(totals[0])
    late[pl.ds(1, 1)] = column_sum(totals[1])
    strip_sum = column_sum(totals[2])
    for group in range(table.shape[0]):
        late[pl.ds(4 + group, 1)] = jnp.where(own_script == group, strip_sum, 0.0)
    share_late = share(1, late, late_in)
    share_late[0](0)
    for j in range(strips):
        xin[j] = res[pl.ds(j * row_count, row_count)].astype(BF)
    from_grad = exchange(3, xin, grad_patches)
    launch(from_grad)
    red.step(PLAN["last"][1:])
    tail = PLAN["tail"]
    turns = [len(tail) * (turn + 1) // 4 for turn in range(3)]
    for index in range(len(tail)):
        red.step(tail[index : index + 1])
        for turn in range(3):
            if turns[turn] == index:
                share_late[1](turn)

    owner = s * strips + q
    spread = lax.broadcasted_iota(jnp.int32, (width, 128), 0)
    lane = lax.broadcasted_iota(jnp.int32, (width, 128), 1)
    few = jnp.where((spread == PART * owner + lane) & (lane < PART), 1.0, 0.0)
    many = jnp.where((spread == 4 * PART * (owner % 8) + lane) & (lane < 4 * PART), 1.0, 0.0)
    exact = lambda left, right: lax.dot_general(
        left, right, (((1,), (0,)), ((), ())), precision=lax.Precision.HIGHEST,
        preferred_element_type=F32,
    )
    lines = lax.broadcasted_iota(jnp.int32, (8, width), 0)
    chosen = jnp.where(lines == 4 + owner // 8, early[...], 0.0)
    small[pl.ds(0, 8)] = exact(early[...], few)
    small[pl.ds(8, 8)] = exact(late[...], few)
    small[pl.ds(16, 8)] = exact(chosen, many)

    red.finish()
    for moves in (from_out, from_grad):
        arrive(moves)
        sent(moves)


def run_layer(*arrays):
    patches = arrays[12]
    row_count, strips, width = patches.shape
    rows = -(-strips * row_count // BLOCK) * BLOCK
    vmem = pl.BlockSpec(memory_space=pltpu.VMEM)
    smem = pl.BlockSpec(memory_space=pltpu.SMEM)
    hbm = pl.BlockSpec(memory_space=pl.ANY)
    packed = lambda *shape: pltpu.VMEM(shape, BF)
    wide = lambda *shape: pltpu.VMEM(shape, F32)
    return pl.pallas_call(
        layer_kernel,
        out_shape=[
            jax.ShapeDtypeStruct((strips, row_count, width), BF),
            jax.ShapeDtypeStruct((strips, row_count, width), BF),
            jax.ShapeDtypeStruct((OWN, PART, WIDE), F32),
            jax.ShapeDtypeStruct((2, 4 * PART, WIDE), F32),
            jax.ShapeDtypeStruct((24, 128), F32),
        ],
        in_specs=[smem] * 2 + [vmem] * 12 + [hbm] * 4,
        out_specs=[hbm, hbm, vmem, vmem, vmem],
        scratch_shapes=[
            packed(strips, row_count, width),
            packed(strips, row_count, width),
            packed(strips, row_count, width),
            wide(rows, width),
            packed(rows, width),
            packed(rows, 3 * width),
            packed(rows, width),
            wide(rows, 128),
            wide(rows, width),
            packed(rows, width),
            packed(rows, width),
            wide(rows, width),
            wide(rows, width),
            packed(rows, width),
            packed(rows, width),
            packed(rows, width),
            packed(rows, width),
            packed(width, width),
            wide(8, width),
            wide(8, width),
            wide(8, width),
            wide(8, width),
            packed(width, 3 * width),
            packed(width, width),
            packed(2, width, width),
            packed(2, width, width),
            packed(2 * SLOTS, 2, 384, WIDE),
            packed(CHUNKS, 384, WIDE),
            packed(CHUNKS, 192, WIDE),
            packed(CHUNKS, 96, WIDE),
            packed(OWN, 48, WIDE),
            packed(OWN, 2, 24, WIDE),
            packed(OWN, 24, WIDE),
            packed(CHUNKS - OWN, 96, WIDE),
            packed(CHUNKS - OWN, 96, WIDE),
        ]
        + [wide(7, 8, width)] * 2
        + [
            pltpu.SemaphoreType.DMA((STAGES, CHUNKS)),
            pltpu.SemaphoreType.DMA((STAGES, CHUNKS)),
            pltpu.SemaphoreType.DMA((2, 7)),
            pltpu.SemaphoreType.DMA((2, 7)),
            pltpu.SemaphoreType.DMA((4, strips)),
            pltpu.SemaphoreType.DMA((4, strips)),
            pltpu.SemaphoreType.DMA((2,)),
            pltpu.SemaphoreType.DMA((2, 2)),
            pltpu.SemaphoreType.DMA((4,)),
        ],
        compiler_params=pltpu.CompilerParams(
            collective_id=0, has_side_effects=True, vmem_limit_bytes=67043328
        ),
    )(*arrays)


def finish_kernel(
    layer_in, grad_in, reduced, reduced_down, small,
    layer_out, grad_patches, table, gain_one, bias_one, qkv, query_bias, value_bias, out_weight,
    out_bias, gain_two, bias_two, up_weight, up_bias, down_weight, down_bias,
):
    for j in range(layer_in.shape[0]):
        layer_out[:, j, :] = layer_in[j]
        grad_patches[:, j, :] = grad_in[j]
    names = {
        0: gain_two, 1: bias_two, 2: out_bias, 3: down_bias,
        8: gain_one, 9: bias_one, 10: query_bias, 11: value_bias,
    }
    for index, ref in names.items():
        ref[...] = small[pl.ds(index, 1), pl.ds(0, PART)].reshape(PART)
    up_bias[...] = column_sum(small[pl.ds(16, 8), pl.ds(0, 4 * PART)]).reshape(4 * PART)
    table[...] = small[pl.ds(12, 4), pl.ds(0, PART)]
    for c in range(8):
        up_weight[:, pl.ds(c * WIDE, WIDE)] = reduced[c]
    for c in range(2):
        out_weight[:, pl.ds(c * WIDE, WIDE)] = reduced[8 + c]
    for half in range(2):
        down_weight[:, pl.ds(half * WIDE, WIDE)] = reduced_down[half]
    width = qkv.shape[1] // 3
    for pair in range(6):
        for part in range(3):
            qkv[:, pl.ds(part * width + pair * 128, 128)] = reduced[
                10 + pair, :, pl.ds(part * 128, 128)
            ]


def local(
    patches,
    lengths,
    script,
    script_table,
    gain_one,
    bias_one,
    qkv_weight,
    query_bias,
    value_bias,
    out_weight,
    out_bias,
    gain_two,
    bias_two,
    up_weight,
    up_bias,
    down_weight,
    down_bias,
    cotangent,
):
    strips, row_count, width = patches.shape
    groups = script_table.shape[0]
    results = run_layer(
        lengths, script, script_table, gain_one, bias_one, query_bias, value_bias, out_bias,
        gain_two, bias_two, up_bias, down_bias, patches.transpose(1, 0, 2),
        cotangent.transpose(1, 0, 2), qkv_weight,
        out_weight, up_weight, down_weight,
    )
    vector = jax.ShapeDtypeStruct((PART,), F32)
    turned = jax.ShapeDtypeStruct((row_count, strips, width), BF)
    outputs = pl.pallas_call(
        finish_kernel,
        out_shape=[
            turned,
            turned,
            jax.ShapeDtypeStruct((groups, PART), F32),
            vector,
            vector,
            jax.ShapeDtypeStruct((PART, 3 * width), F32),
            vector,
            vector,
            jax.ShapeDtypeStruct((PART, width), F32),
            vector,
            vector,
            vector,
            jax.ShapeDtypeStruct((PART, up_weight.shape[1]), F32),
            jax.ShapeDtypeStruct((4 * PART,), F32),
            jax.ShapeDtypeStruct((4 * PART, width), F32),
            vector,
        ],
    )(*results)
    return (
        outputs[0].transpose(1, 0, 2),
        outputs[1].transpose(1, 0, 2),
        outputs[2].T,
        *outputs[3:],
    )


def solution(mesh):
    placed = (
        P("strip", "seq", None),
        P("strip"),
        P("strip"),
        P(),
        P(),
        P(),
        P(),
        P(),
        P(),
        P(),
        P(),
        P(),
        P(),
        P(),
        P(),
        P(),
        P(),
        P("strip", "seq", None),
    )
    chosen = local if fits(mesh) else local_general
    return jax.shard_map(
        chosen,
        mesh=mesh,
        in_specs=placed,
        out_specs=(
            P("strip", "seq", None),
            P("strip", "seq", None),
            P(("strip", "seq"), None),
            P(("strip", "seq")),
            P(("strip", "seq")),
            P(("strip", "seq"), None),
            P(("strip", "seq")),
            P(("strip", "seq")),
            P(("strip", "seq"), None),
            P(("strip", "seq")),
            P(("strip", "seq")),
            P(("strip", "seq")),
            P(("strip", "seq"), None),
            P(("strip", "seq")),
            P(("strip", "seq"), None),
            P(("strip", "seq")),
        ),
        check_vma=False,
    )
```

```python
import functools

import jax
import jax.numpy as jnp
from jax import lax
from jax.experimental import pallas as pl
from jax.experimental.pallas import tpu as pltpu
from jax.sharding import PartitionSpec as P

HD = 64


epsilon = 1e-12


def normalize(hidden):
    centred = hidden - jnp.mean(hidden, axis=-1, keepdims=True)
    inverse = lax.rsqrt(jnp.mean(centred * centred, axis=-1, keepdims=True) + epsilon)
    return (centred * inverse, inverse)


def norm_back(upstream, gain, normed, inverse):
    scaled = upstream * gain
    return inverse * (
        scaled
        - jnp.mean(scaled, axis=-1, keepdims=True)
        - normed * jnp.mean(scaled * normed, axis=-1, keepdims=True)
    )


def weight_grad(inputs, upstream):
    return lax.dot_general(
        inputs, upstream, (((0,), (0,)), ((), ())), preferred_element_type=jnp.float32
    )


def input_grad(upstream, weight):
    return lax.dot_general(
        upstream, weight, (((1,), (1,)), ((), ())), preferred_element_type=jnp.float32
    )


def gelu_slope(upper):
    return (
        0.5 * (1.0 + lax.erf(upper * 0.7071067811865476))
        + upper * jnp.exp(-0.5 * upper * upper) * 0.3989422804014327
    )


def split_block(block):
    seq_len = block.shape[0]
    heads_here = block.shape[2] // HD
    return [block[:, member].reshape(seq_len, heads_here, HD) for member in range(3)]


def masked_logits(queries, key_rows, length):
    logits = jnp.einsum(
        "qhd,khd->hqk", queries, key_rows, preferred_element_type=jnp.float32
    ) * HD ** (-0.5)
    visible = jnp.arange(logits.shape[-1], dtype=jnp.int32) < length
    return jnp.where(visible[None, None, :], logits, -1000000000.0)


def attend_forward(item):
    block, length = item
    queries, key_rows, values = split_block(block)
    logits = masked_logits(queries, key_rows, length)
    highest = jnp.max(logits, axis=-1, keepdims=True)
    expanded = jnp.exp(logits - highest)
    totals = jnp.sum(expanded, axis=-1, keepdims=True)
    probs = (expanded / totals).astype(jnp.bfloat16)
    mixed = jnp.einsum("hqk,khd->qhd", probs, values, preferred_element_type=jnp.float32)
    mixed = mixed.astype(jnp.bfloat16).reshape(block.shape[0], block.shape[2])
    return (mixed, (highest + jnp.log(totals))[..., 0])


def attend_backward(item):
    block, log_total, grad_mixed, length = item
    queries, key_rows, values = split_block(block)
    logits = masked_logits(queries, key_rows, length)
    probs = jnp.exp(logits - log_total[..., None])
    grad_heads = grad_mixed.reshape(queries.shape)
    grad_values = jnp.einsum(
        "hqk,qhd->khd", probs.astype(jnp.bfloat16), grad_heads, preferred_element_type=jnp.float32
    )
    grad_probs = jnp.einsum("qhd,khd->hqk", grad_heads, values, preferred_element_type=jnp.float32)
    inner = jnp.sum(probs * grad_probs, axis=-1, keepdims=True)
    grad_logits = (probs * (grad_probs - inner)).astype(jnp.bfloat16)
    grad_queries = jnp.einsum(
        "hqk,khd->qhd", grad_logits, key_rows, preferred_element_type=jnp.float32
    ) * HD ** (-0.5)
    grad_keys = jnp.einsum(
        "hqk,qhd->khd", grad_logits, queries, preferred_element_type=jnp.float32
    ) * HD ** (-0.5)
    stacked = jnp.stack([grad_queries, grad_keys, grad_values], axis=1)
    return stacked.reshape(block.shape).astype(jnp.bfloat16)


def local_general(
    patches,
    lengths,
    script,
    script_table,
    gain_one,
    bias_one,
    qkv_weight,
    query_bias,
    value_bias,
    out_weight,
    out_bias,
    gain_two,
    bias_two,
    up_weight,
    up_bias,
    down_weight,
    down_bias,
    cotangent,
):
    strips, row_count, model_width = patches.shape
    groups = script_table.shape[0]
    tokens = strips * row_count
    selector = (script[:, None] == jnp.arange(groups, dtype=jnp.int32)[None, :]).astype(jnp.float32)
    added = jnp.dot(selector.astype(jnp.bfloat16), script_table, preferred_element_type=jnp.float32)
    hidden = (patches.astype(jnp.float32) + added[:, None, :]).reshape(tokens, model_width)
    normed_one, inverse_one = normalize(hidden)
    inputs_one = (normed_one * gain_one + bias_one).astype(jnp.bfloat16)
    joint_bias = jnp.concatenate([query_bias, jnp.zeros_like(query_bias), value_bias])
    projected = (
        jnp.dot(inputs_one, qkv_weight, preferred_element_type=jnp.float32) + joint_bias
    ).astype(jnp.bfloat16)
    projected = projected.reshape(strips, row_count, 3, model_width)
    head_blocks = lax.all_to_all(projected, "seq", split_axis=3, concat_axis=1, tiled=True)
    mixed_heads, log_totals = lax.map(attend_forward, (head_blocks, lengths))
    mixed = lax.all_to_all(mixed_heads, "seq", split_axis=1, concat_axis=2, tiled=True).reshape(
        tokens, model_width
    )
    attended = hidden + jnp.dot(mixed, out_weight, preferred_element_type=jnp.float32) + out_bias
    normed_two, inverse_two = normalize(attended)
    inputs_two = (normed_two * gain_two + bias_two).astype(jnp.bfloat16)
    upper = jnp.dot(inputs_two, up_weight, preferred_element_type=jnp.float32) + up_bias
    active = jax.nn.gelu(upper, approximate=False).astype(jnp.bfloat16)
    result = attended + jnp.dot(active, down_weight, preferred_element_type=jnp.float32) + down_bias
    layer_out = result.astype(jnp.bfloat16).reshape(strips, row_count, model_width)
    grad_result = cotangent.reshape(tokens, model_width)
    grad_float = grad_result.astype(jnp.float32)
    grad_down_weight = weight_grad(active, grad_result)
    grad_down_bias = jnp.sum(grad_float, axis=0)
    grad_upper = (input_grad(grad_result, down_weight) * gelu_slope(upper)).astype(jnp.bfloat16)
    grad_up_weight = weight_grad(inputs_two, grad_upper)
    grad_up_bias = jnp.sum(grad_upper.astype(jnp.float32), axis=0)
    grad_inputs_two = input_grad(grad_upper, up_weight)
    grad_gain_two = jnp.sum(grad_inputs_two * normed_two, axis=0)
    grad_bias_two = jnp.sum(grad_inputs_two, axis=0)
    grad_attended = grad_float + norm_back(grad_inputs_two, gain_two, normed_two, inverse_two)
    grad_branch = grad_attended.astype(jnp.bfloat16)
    grad_out_weight = weight_grad(mixed, grad_branch)
    grad_out_bias = jnp.sum(grad_branch.astype(jnp.float32), axis=0)
    grad_mixed = (
        input_grad(grad_branch, out_weight)
        .astype(jnp.bfloat16)
        .reshape(strips, row_count, model_width)
    )
    grad_mixed_heads = lax.all_to_all(grad_mixed, "seq", split_axis=2, concat_axis=1, tiled=True)
    grad_heads = lax.map(attend_backward, (head_blocks, log_totals, grad_mixed_heads, lengths))
    grad_projected = lax.all_to_all(
        grad_heads, "seq", split_axis=1, concat_axis=3, tiled=True
    ).reshape(tokens, 3 * model_width)
    grad_qkv = weight_grad(inputs_one, grad_projected)
    grad_bias_rows = jnp.sum(grad_projected.astype(jnp.float32), axis=0)
    grad_query_bias = grad_bias_rows[:model_width]
    grad_value_bias = grad_bias_rows[2 * model_width :]
    grad_inputs_one = input_grad(grad_projected, qkv_weight)
    grad_gain_one = jnp.sum(grad_inputs_one * normed_one, axis=0)
    grad_bias_one = jnp.sum(grad_inputs_one, axis=0)
    grad_hidden = grad_attended + norm_back(grad_inputs_one, gain_one, normed_one, inverse_one)
    grad_patches = grad_hidden.astype(jnp.bfloat16).reshape(strips, row_count, model_width)
    per_strip = jnp.sum(grad_hidden.reshape(strips, row_count, model_width), axis=1)
    grad_table = jnp.dot(per_strip.T, selector, precision=lax.Precision.HIGHEST)
    summed = (
        lax.psum_scatter(grad_table, ("strip", "seq"), scatter_dimension=0, tiled=True),
        lax.psum_scatter(grad_gain_one, ("strip", "seq"), scatter_dimension=0, tiled=True),
        lax.psum_scatter(grad_bias_one, ("strip", "seq"), scatter_dimension=0, tiled=True),
        lax.psum_scatter(grad_qkv, ("strip", "seq"), scatter_dimension=0, tiled=True),
        lax.psum_scatter(grad_query_bias, ("strip", "seq"), scatter_dimension=0, tiled=True),
        lax.psum_scatter(grad_value_bias, ("strip", "seq"), scatter_dimension=0, tiled=True),
        lax.psum_scatter(grad_out_weight, ("strip", "seq"), scatter_dimension=0, tiled=True),
        lax.psum_scatter(grad_out_bias, ("strip", "seq"), scatter_dimension=0, tiled=True),
        lax.psum_scatter(grad_gain_two, ("strip", "seq"), scatter_dimension=0, tiled=True),
        lax.psum_scatter(grad_bias_two, ("strip", "seq"), scatter_dimension=0, tiled=True),
        lax.psum_scatter(grad_up_weight, ("strip", "seq"), scatter_dimension=0, tiled=True),
        lax.psum_scatter(grad_up_bias, ("strip", "seq"), scatter_dimension=0, tiled=True),
        lax.psum_scatter(grad_down_weight, ("strip", "seq"), scatter_dimension=0, tiled=True),
        lax.psum_scatter(grad_down_bias, ("strip", "seq"), scatter_dimension=0, tiled=True),
    )
    return (
        layer_out,
        grad_patches,
        summed[0],
        summed[1],
        summed[2],
        summed[3],
        summed[4],
        summed[5],
        summed[6],
        summed[7],
        summed[8],
        summed[9],
        summed[10],
        summed[11],
        summed[12],
        summed[13],
    )


MESH = pl.DeviceIdType.MESH
BF = jnp.bfloat16
F32 = jnp.float32
CHUNKS = 24
OWN = 16
SLOTS = 4
STAGES = 5
WIDE = 384
PART = 24
BLOCK = 32

PLAN = {
    "ffn": [
        [
            (0, 0, 0, 0, 0, 0, 0, 0, 0, 0, 0, 0, 0, 0, 0, 0, 0, 0, 0, 0),
            (0, 0, 0, 0, 0, 0, 0, 0, 0, 0, 2, 0, 0, 0, 0, 2, 0, 0, 0, 0),
            (2, 0, 0, 0, 0, 2, 0, 0, 0, 0, 4, 2, 0, 0, 0, 4, 1, 0, 0, 0),
            (4, 2, 0, 0, 0, 4, 2, 0, 0, 0, 6, 2, 2, 0, 0, 6, 2, 1, 0, 0),
        ],
        [
            (0, 0, 0, 0, 0, 0, 0, 0, 0, 0, 0, 0, 0, 0, 0, 0, 0, 0, 0, 0),
            (2, 0, 0, 0, 0, 2, 0, 0, 0, 0, 2, 0, 0, 0, 0, 2, 0, 0, 0, 0),
            (4, 2, 0, 0, 0, 4, 1, 0, 0, 0, 4, 2, 0, 0, 0, 4, 1, 0, 0, 0),
            (6, 2, 2, 0, 0, 6, 2, 1, 0, 0, 6, 4, 2, 0, 0, 6, 2, 1, 0, 0),
        ],
        [
            (0, 0, 0, 0, 0, 0, 0, 0, 0, 0, 0, 0, 0, 0, 0, 0, 0, 0, 0, 0),
            (2, 0, 0, 0, 0, 2, 0, 0, 0, 0, 2, 0, 0, 0, 0, 2, 0, 0, 0, 0),
            (4, 2, 0, 0, 0, 4, 1, 0, 0, 0, 4, 2, 0, 0, 0, 4, 2, 0, 0, 0),
            (6, 4, 2, 0, 0, 6, 2, 1, 0, 0, 6, 4, 2, 0, 0, 6, 3, 1, 0, 0),
        ],
    ],
    "after": [
        (6, 4, 2, 0, 0, 6, 3, 1, 0, 0, 8, 4, 2, 2, 0, 7, 4, 2, 1, 0),
        (8, 4, 2, 2, 0, 7, 4, 2, 1, 0, 8, 4, 2, 2, 0, 8, 5, 2, 1, 0),
        (8, 4, 2, 2, 0, 8, 5, 2, 1, 0, 8, 6, 3, 2, 0, 8, 5, 2, 1, 0),
    ],
    "pair": [
        (8, 6, 3, 2, 0, 8, 5, 2, 1, 0, 10, 6, 4, 2, 2, 8, 6, 2, 2, 1),
        (10, 6, 4, 2, 2, 8, 6, 2, 2, 1, 10, 6, 4, 3, 2, 8, 6, 3, 2, 1),
        (10, 8, 4, 3, 2, 8, 6, 3, 2, 2, 12, 8, 4, 3, 3, 8, 6, 5, 3, 2),
        (12, 8, 4, 3, 3, 8, 6, 5, 3, 2, 12, 10, 4, 4, 3, 8, 8, 5, 3, 2),
        (12, 10, 6, 4, 3, 8, 8, 5, 5, 3, 14, 12, 7, 4, 3, 8, 8, 7, 5, 3),
        (14, 12, 7, 4, 3, 8, 8, 7, 5, 3, 14, 12, 9, 7, 4, 8, 8, 7, 5, 4),
    ],
    "grad": [
        [
            (10, 6, 4, 3, 2, 8, 6, 3, 2, 1, 10, 8, 4, 3, 2, 8, 6, 3, 2, 1),
            (12, 10, 4, 4, 3, 8, 8, 5, 3, 2, 12, 10, 5, 4, 3, 8, 8, 5, 3, 2),
            (14, 12, 9, 7, 4, 8, 8, 7, 5, 4, 14, 12, 10, 7, 4, 8, 8, 7, 6, 5),
        ],
        [
            (10, 8, 4, 3, 2, 8, 6, 3, 2, 1, 10, 8, 4, 3, 2, 8, 6, 3, 2, 2),
            (12, 10, 5, 4, 3, 8, 8, 5, 3, 2, 12, 10, 6, 4, 3, 8, 8, 5, 5, 3),
            (14, 12, 10, 7, 4, 8, 8, 7, 6, 5, 14, 13, 10, 7, 4, 8, 8, 8, 7, 5),
        ],
    ],
    "last": [
        (14, 13, 10, 7, 4, 8, 8, 8, 7, 5, 16, 14, 11, 8, 4, 8, 8, 8, 7, 5),
        (16, 14, 11, 8, 4, 8, 8, 8, 7, 5, 16, 14, 12, 8, 5, 8, 8, 8, 7, 5),
    ],
    "tail": [
        (16, 14, 12, 8, 5, 8, 8, 8, 7, 5, 16, 14, 12, 10, 7, 8, 8, 8, 7, 5),
        (16, 14, 12, 10, 7, 8, 8, 8, 7, 5, 16, 14, 13, 10, 7, 8, 8, 8, 7, 5),
        (16, 14, 13, 10, 7, 8, 8, 8, 7, 5, 16, 14, 13, 10, 7, 8, 8, 8, 7, 6),
        (16, 14, 13, 10, 7, 8, 8, 8, 7, 6, 16, 14, 14, 10, 7, 8, 8, 8, 8, 6),
        (16, 14, 14, 10, 7, 8, 8, 8, 8, 6, 16, 14, 14, 11, 7, 8, 8, 8, 8, 7),
        (16, 14, 14, 11, 7, 8, 8, 8, 8, 7, 16, 14, 14, 11, 8, 8, 8, 8, 8, 7),
        (16, 14, 14, 11, 8, 8, 8, 8, 8, 7, 16, 15, 14, 11, 8, 8, 8, 8, 8, 7),
        (16, 15, 14, 11, 8, 8, 8, 8, 8, 7, 16, 15, 14, 12, 8, 8, 8, 8, 8, 7),
        (16, 15, 14, 12, 8, 8, 8, 8, 8, 7, 16, 16, 14, 12, 8, 8, 8, 8, 8, 7),
        (16, 16, 14, 12, 8, 8, 8, 8, 8, 7, 16, 16, 14, 12, 9, 8, 8, 8, 8, 7),
        (16, 16, 14, 12, 9, 8, 8, 8, 8, 7, 16, 16, 14, 14, 9, 8, 8, 8, 8, 7),
        (16, 16, 14, 14, 9, 8, 8, 8, 8, 7, 16, 16, 14, 14, 10, 8, 8, 8, 8, 7),
        (16, 16, 14, 14, 10, 8, 8, 8, 8, 7, 16, 16, 15, 14, 10, 8, 8, 8, 8, 7),
        (16, 16, 15, 14, 10, 8, 8, 8, 8, 7, 16, 16, 15, 14, 11, 8, 8, 8, 8, 7),
        (16, 16, 15, 14, 11, 8, 8, 8, 8, 7, 16, 16, 16, 14, 12, 8, 8, 8, 8, 8),
        (16, 16, 16, 14, 12, 8, 8, 8, 8, 8, 16, 16, 16, 14, 13, 8, 8, 8, 8, 8),
        (16, 16, 16, 14, 13, 8, 8, 8, 8, 8, 16, 16, 16, 15, 14, 8, 8, 8, 8, 8),
        (16, 16, 16, 15, 14, 8, 8, 8, 8, 8, 16, 16, 16, 16, 14, 8, 8, 8, 8, 8),
        (16, 16, 16, 16, 14, 8, 8, 8, 8, 8, 16, 16, 16, 16, 15, 8, 8, 8, 8, 8),
        (16, 16, 16, 16, 15, 8, 8, 8, 8, 8, 16, 16, 16, 16, 16, 8, 8, 8, 8, 8),
    ],
}


def fits(mesh):
    return dict(mesh.shape) == {"strip": 8, "seq": 4}


def dot(left, right, left_dim, right_dim):
    return lax.dot_general(
        left, right, (((left_dim,), (right_dim,)), ((), ())), preferred_element_type=F32
    )


def mean(block):
    return jnp.mean(block, axis=1, keepdims=True)


def fold(block):
    return jnp.sum(block.reshape(block.shape[0] // 8, 8, block.shape[1]), axis=0)


def sweep(blocks, body, totals, first=0):
    def trip(start, size, totals):
        results = [body(start + k) for k in range(size)]
        for stores, _ in results:
            for ref, at, value in stores:
                ref[at] = value
        return tuple(
            total + sum(sums[k] for _, sums in results) for k, total in enumerate(totals)
        )

    whole = (blocks - first) // 4
    totals = lax.fori_loop(0, whole, lambda i, t: trip(first + 4 * i, 4, t), totals)
    if (blocks - first) % 4:
        totals = trip(first + 4 * whole, (blocks - first) % 4, totals)
    return totals


def block_rows(b):
    if isinstance(b, int):
        return pl.ds(b * BLOCK, BLOCK)
    return pl.ds(pl.multiple_of(b * BLOCK, BLOCK), BLOCK)


def column_sum(block):
    return jnp.sum(block, axis=0, keepdims=True)


def attend_pair(pair, visible, proj, mixed, lse_all):
    width = proj.shape[1] // 3
    at = lambda part: pl.ds(pl.multiple_of(part * width + pair * 128, 128), 128)
    lane = lax.broadcasted_iota(jnp.int32, (1, 128), 1)
    q = proj[:, at(0)] * jnp.asarray(0.125, BF)
    k = proj[:, at(1)]
    v = proj[:, at(2)]
    outs, logs = [], []
    for head in range(2):
        own = (lane // HD) == head
        logits = dot(jnp.where(own, q, jnp.zeros_like(q)), k, 1, 1)
        logits = jnp.where(visible, logits, -1000000000.0)
        highest = jnp.max(logits, axis=1, keepdims=True)
        expanded = jnp.exp(logits - highest)
        total = jnp.sum(expanded, axis=1, keepdims=True)
        probs = (expanded * (1.0 / total)).astype(BF)
        outs.append(dot(probs, v, 1, 0))
        logs.append(highest + jnp.log(total))
    mixed[:, at(0)] = jnp.where(lane < HD, outs[0], outs[1]).astype(BF)
    known = jnp.where(lane == 2 * pair, logs[0], lse_all[...])
    lse_all[...] = jnp.where(lane == 2 * pair + 1, logs[1], known)


def attend_pair_back(pair, visible, proj, gmixed, lse_all):
    width = proj.shape[1] // 3
    at = lambda part: pl.ds(pl.multiple_of(part * width + pair * 128, 128), 128)
    lane = lax.broadcasted_iota(jnp.int32, (1, 128), 1)
    q = proj[:, at(0)] * jnp.asarray(0.125, BF)
    k = proj[:, at(1)]
    v = proj[:, at(2)]
    gm = gmixed[:, at(0)]
    lse = lse_all[...]
    grads = []
    for head in range(2):
        own = (lane // HD) == head
        q_own = jnp.where(own, q, jnp.zeros_like(q))
        g_own = jnp.where(own, gm, jnp.zeros_like(gm))
        k_own = jnp.where(own, k, jnp.zeros_like(k))
        own_lse = jnp.sum(jnp.where(lane == 2 * pair + head, lse, 0.0), axis=1, keepdims=True)
        logits = dot(q_own, k, 1, 1)
        probs = jnp.where(visible, jnp.exp(logits - own_lse), 0.0)
        grad_probs = dot(g_own, v, 1, 1)
        inner = jnp.sum(probs * grad_probs, axis=1, keepdims=True)
        grad_logits = (probs * (grad_probs - inner)).astype(BF)
        grads.append(
            (
                dot(grad_logits, k_own, 1, 0),
                dot(q_own, grad_logits, 0, 0),
                dot(g_own, probs.astype(BF), 0, 0),
            )
        )
    gq = ((grads[0][0] + grads[1][0]) * 0.125).astype(BF)
    gk = (grads[0][1] + grads[1][1]).T.astype(BF)
    gv = (grads[0][2] + grads[1][2]).T.astype(BF)
    return gq, gk, gv


class Devices:
    def __init__(self):
        s, q = lax.axis_index("strip"), lax.axis_index("seq")
        self.s, self.q = s, q
        self.core, self.y = q % 2, q // 2
        self.x, self.low, self.high = s % 2, (s // 2) % 2, s // 4
        self.to_core = (s, q + 1 - 2 * self.core)
        self.to_y = (s, q + 2 - 4 * self.y)
        self.to_x = (s + 1 - 2 * self.x, q)
        self.to_low = (s + 2 - 4 * self.low, q)
        self.to_high = (s + 4 - 8 * self.high, q)
        self.to_far = (s + 2 - 4 * self.low + 4 - 8 * self.high, q)


def pick(index, values):
    chosen = values[0]
    for position in range(1, len(values)):
        change = values[position] - values[position - 1]
        if change:
            chosen = chosen + jnp.where(index >= position, change, 0)
    return chosen


class Reduction:
    def __init__(self, dev, g, r1, r2, r3, r4, s4, r5, r4d, r5d, write, write_down, send, recv):
        self.dev = dev
        self.bufs = (g, r1, r2, r3, r4, s4, r5, r4d, r5d)
        self.write = write
        self.write_down = write_down
        self.sems = (send, recv)

    def side(self, stage, c, down):
        dev = self.dev
        odd = c % 2
        even = 1 - odd
        if down:
            by_x, by_y, by_low = ((odd, even, 0), (even, odd, 0), (0, 0, 1))[stage - 1]
        else:
            by_x, by_y, by_low = ((even, 0, odd), (0, 1, 0), (odd, 0, even))[stage - 1]
        device = (
            dev.s + by_x * (1 - 2 * dev.x) + by_low * (2 - 4 * dev.low),
            dev.q + by_y * (2 - 4 * dev.y),
        )
        return device, by_x * dev.x + by_y * dev.y + by_low * dev.low

    def slot(self, c, down):
        return c % SLOTS + SLOTS if down else c % SLOTS

    def copy(self, stage, c, down):
        g, r1, r2, r3, r4, s4, r5, r4d, r5d = self.bufs
        dev = self.dev
        if stage == 0:
            source, target = g.at[self.slot(c, down), 1 - dev.core], r1.at[c]
            device = dev.to_core
        elif stage == 4:
            device = dev.to_high
            if down:
                source, target = r4d.at[c - OWN], r5d.at[c - OWN]
            else:
                source, target = s4.at[c, 1 - dev.high], r5.at[c]
        elif stage == 3 and down:
            source, target, device = r3.at[c], r4d.at[c - OWN], dev.to_low
        else:
            device, bit = self.side(stage, c, down)
            rows = 384 >> stage
            held, target = ((r1, r2), (r2, r3), (r3, r4))[stage - 1]
            source, target = held.at[c, pl.ds((1 - bit) * rows, rows)], target.at[c]
        send, recv = self.sems
        return pltpu.make_async_remote_copy(
            src_ref=source,
            dst_ref=target,
            send_sem=send.at[stage, c],
            recv_sem=recv.at[stage, c],
            device_id=device,
            device_id_type=MESH,
        )

    def near(self, c):
        return self.dev.low == (c - OWN) // 2 % 2

    def far(self, c):
        return self.dev.high == (c - OWN) // 4

    def free(self, c, down):
        first = OWN if down else 0

        @pl.when(c >= first + SLOTS)
        def _():
            self.copy(0, c - SLOTS, down).wait_send()

    def start(self, c, down):
        self.copy(0, c, down).start()

    def event(self, stage, c, down):
        g, r1, r2, r3, r4, s4, r5, r4d, r5d = self.bufs
        dev = self.dev
        if stage >= 3 and down:
            self.last_events(stage, c)
            return
        self.copy(stage, c, down).wait_recv()
        if stage == 0:
            slot = self.slot(c, down)

            @pl.loop(0, 2)
            def _(i):
                rows = pl.ds(pl.multiple_of(i * 192, 192), 192)
                r1[c, rows] = r1[c, rows] + g[slot, dev.core, rows]
        elif stage < 3:
            _, bit = self.side(stage, c, down)
            held, target = ((r1, r2), (r2, r3))[stage - 1]

            size = 384 >> stage
            kept = pl.ds(pl.multiple_of(bit * size, size), size)
            target[c] = target[c] + held[c, kept]
        elif stage == 3:
            _, bit = self.side(stage, c, down)
            kept = pl.ds(pl.multiple_of(bit * 48, 48), 48)
            total = r4[c].astype(F32) + r3[c, kept].astype(F32)
            s4[c, 0] = total[:24].astype(BF)
            s4[c, 1] = total[24:].astype(BF)
        else:
            self.write[c] = s4[c, dev.high].astype(F32) + r5[c].astype(F32)
            return
        if stage == 2 and down:

            @pl.when(jnp.logical_not(self.near(c)))
            def _():
                self.copy(3, c, down).start()
        else:
            self.copy(stage + 1, c, down).start()

    def last_events(self, stage, c):
        r3, r4d, r5d = self.bufs[3], self.bufs[7], self.bufs[8]

        @pl.when(self.near(c))
        def _():
            if stage == 3:
                self.copy(3, c, True).wait_recv()
                r4d[c - OWN] = r4d[c - OWN] + r3[c]

                @pl.when(jnp.logical_not(self.far(c)))
                def _():
                    self.copy(4, c, True).start()
            else:

                @pl.when(self.far(c))
                def _():
                    self.copy(4, c, True).wait_recv()
                    total = r4d[c - OWN].astype(F32) + r5d[c - OWN].astype(F32)
                    self.write_down[c % 2] = total

    def step(self, plans, index=0):
        for column in (4, 9, 3, 8, 2, 7, 1, 6, 0, 5):
            low = pick(index, [plan[column] for plan in plans])
            high = pick(index, [plan[2 * STAGES + column] for plan in plans])
            if all(plan[column] == plan[2 * STAGES + column] for plan in plans):
                continue
            down = column >= STAGES
            first = OWN if down else 0

            @pl.loop(low + first, high + first)
            def _(c):
                self.event(column % STAGES, c, down)

    def finish(self):
        for down in (False, True):
            first, last = (OWN, CHUNKS) if down else (0, OWN)

            @pl.loop(last - SLOTS, last)
            def _(c):
                self.copy(0, c, down).wait_send()

            @pl.loop(first, last)
            def _(c):
                for stage in range(1, STAGES):
                    if down and stage == 3:

                        @pl.when(jnp.logical_not(self.near(c)))
                        def _():
                            self.copy(3, c, True).wait_send()
                    elif down and stage == 4:

                        @pl.when(self.near(c) & jnp.logical_not(self.far(c)))
                        def _():
                            self.copy(4, c, True).wait_send()
                    else:
                        self.copy(stage, c, down).wait_send()

    def place(self, c, half, product):
        columns = pl.ds(half * WIDE, WIDE)
        for owner in range(32):
            core, y, x, low, high = [(owner >> bit) % 2 for bit in range(5)]
            unit = 4 * low + 2 * y + x if half else 4 * x + 2 * y + low
            self.bufs[0][self.slot(c, False), core, pl.ds(unit * 48 + high * PART, PART)] = product[
                pl.ds(owner * PART, PART), columns
            ]

    def place_down(self, c, half, product):
        columns = pl.ds(half * WIDE, WIDE)
        for owner in range(8):
            core, y, x = [(owner >> bit) % 2 for bit in range(3)]
            unit = 2 * x + y if half else 2 * y + x
            self.bufs[0][self.slot(c, True), core, pl.ds(unit * 96, 96)] = product[
                pl.ds(owner * 96, 96), columns
            ]


ERF_TOP = (
    0.00022905065861350646, 0.0034082910107109506, 0.050955695062380861, 0.18520832239976145,
    1.128379143519084,
)
ERF_BOTTOM = (
    -1.1791602954361697e-7, 0.000023547966471313185, 0.0010179625278914885,
    0.014070470171167667, 0.11098505178285362, 0.49746925110067538, 1.0,
)


def erf(value):
    value = jnp.clip(value, -3.832506856900711, 3.832506856900711)
    square = value * value
    top = jnp.full_like(square, ERF_TOP[0])
    for term in ERF_TOP[1:]:
        top = top * square + term
    bottom = jnp.full_like(square, ERF_BOTTOM[0])
    for term in ERF_BOTTOM[1:]:
        bottom = bottom * square + term
    return value * top / bottom


def standardize(block):
    centred = block - mean(block)
    inverse = lax.rsqrt(mean(centred * centred) + epsilon)
    return centred * inverse, inverse


def layer_kernel(
    lengths, script, table, gain_one, bias_one, query_bias, value_bias, out_bias, gain_two,
    bias_two, up_bias, down_bias, patches, cotangent, qkv_hbm, out_hbm, up_hbm, down_hbm,
    layer_out, grad_patches, reduced, reduced_down, small,
    outgoing, xin, cin, hidden, n1, proj, mixed, lse_all, att, n2, cot, res, gn, branch, gmixed,
    gblk, act, product, jbias, ubias, early, late, wqkv, wout, wup, wdown,
    g, r1, r2, r3, r4, s4, r5, r4d, r5d, early_in, late_in,
    send, recv, vsend, vrecv, xsend, xrecv, wsem, fsem, osem,
):
    row_count, strips, width = patches.shape
    count = strips * row_count
    rows = hidden.shape[0]
    blocks = rows // BLOCK
    ff_blocks = up_hbm.shape[1] // width
    dev = Devices()
    s, q = dev.s, dev.q
    red = Reduction(
        dev, g, r1, r2, r3, r4, s4, r5, r4d, r5d, reduced, reduced_down, send, recv
    )

    barrier = pltpu.get_barrier_semaphore()
    greeted = [(s, (q + hop) % strips) for hop in range(1, strips)]
    greeted += [dev.to_x, dev.to_low, dev.to_high, dev.to_far]
    for device in greeted:
        pl.semaphore_signal(barrier, inc=1, device_id=device, device_id_type=MESH)

    load_qkv = pltpu.make_async_copy(qkv_hbm, wqkv, wsem.at[0])
    load_out = pltpu.make_async_copy(out_hbm, wout, wsem.at[1])

    def load_ff(block):
        columns = pl.ds(pl.multiple_of(block * width, width), width)
        slot = block % 2
        return (
            pltpu.make_async_copy(up_hbm.at[:, columns], wup.at[slot], fsem.at[0, slot]),
            pltpu.make_async_copy(down_hbm.at[columns], wdown.at[slot], fsem.at[1, slot]),
        )

    def exchange(group, source, target):
        near, across = q + 1 - 2 * dev.core, q + 2 - 4 * dev.y
        copies = []
        for k, other in enumerate((near, across, near + 2 - 4 * dev.y)):
            copies.append(
                pltpu.make_async_remote_copy(
                    src_ref=source.at[other],
                    dst_ref=target.at[q],
                    send_sem=xsend.at[group, k],
                    recv_sem=xrecv.at[group, k],
                    device_id=(s, other),
                    device_id_type=MESH,
                )
            )
        own = pltpu.make_async_copy(source.at[q], target.at[q], osem.at[group])
        return copies, own

    def launch(moves):
        copies, own = moves
        for index in (1, 2, 0):
            copies[index].start()
        own.start()

    def order(m):
        return (2 * dev.y + m) % strips

    def seen():
        local = lax.broadcasted_iota(jnp.int32, (1, rows), 1)
        shift = jnp.where(local < count // 2, count // 2, -(count // 2)) * dev.y
        return (local + shift < length) & (local < count)

    def arrive(moves):
        copies, own = moves
        for copy in copies:
            copy.wait_recv()
        own.wait()

    def share(group, total, arrived):
        steps = [
            [(s, (q + hop) % strips) for hop in range(1, strips)],
            [dev.to_x],
            [dev.to_low, dev.to_high, dev.to_far],
        ]

        def copies(step):
            first = (0, 3, 4)[step]
            return [
                pltpu.make_async_remote_copy(
                    src_ref=total,
                    dst_ref=arrived.at[first + k],
                    send_sem=vsend.at[group, first + k],
                    recv_sem=vrecv.at[group, first + k],
                    device_id=device,
                    device_id_type=MESH,
                )
                for k, device in enumerate(steps[step])
            ]

        def begin(step):
            for copy in copies(step):
                copy.start()

        def end(step):
            first = (0, 3, 4)[step]
            moves = copies(step)
            for copy in moves:
                copy.wait_recv()
            for copy in moves:
                copy.wait_send()
            total[...] = total[...] + sum(arrived[first + k] for k in range(len(moves)))
            if step < 2:
                begin(step + 1)

        return begin, end

    def sent(moves):
        for copy in moves[0]:
            copy.wait_send()
        return moves

    into_x = exchange(0, outgoing, xin)
    into_c = exchange(1, outgoing, cin)
    for j in range(strips):
        outgoing[j] = patches[:, j, :]
    pl.semaphore_wait(barrier, len(greeted))
    launch(into_x)
    load_qkv.start()
    load_out.start()
    for copy in load_ff(0):
        copy.start()

    length = lengths[q]
    own_script = script[q]
    added = jnp.zeros((1, width), F32)
    for group in range(table.shape[0]):
        added = jnp.where(own_script == group, table[pl.ds(group, 1)].astype(F32), added)
    row = lambda ref: ref[...].reshape(1, ref.shape[0])
    jbias[pl.ds(0, 1)] = row(query_bias)
    jbias[pl.ds(1, 1)] = jnp.zeros((1, width), F32)
    jbias[pl.ds(2, 1)] = row(value_bias)
    hidden[pl.ds(count, rows - count)] = jnp.zeros((rows - count, width), F32)
    gn[pl.ds(count, rows - count)] = jnp.zeros((rows - count, width), F32)
    lse_all[...] = jnp.zeros_like(lse_all)

    for block in range(ff_blocks):
        ubias[pl.ds(block, 1)] = row(up_bias)[:, block * width : block * width + width]

    def first_norm(b):
        at = block_rows(b)
        normed, _ = standardize(hidden[at])
        return [(n1, at, (normed * row(gain_one) + row(bias_one)).astype(BF))], ()

    def project(first, size):
        @pl.loop(0, 3)
        def _(part):
            columns = pl.ds(pl.multiple_of(part * width, width), width)
            made = dot(n1[pl.ds(first, size)], wqkv[:, columns], 1, 0) + jbias[pl.ds(part, 1)]
            proj[pl.ds(first, size), columns] = made.astype(BF)

    into_x[0][0].wait_recv()
    into_x[1].wait()
    for m in range(2):
        hidden[pl.ds(m * row_count, row_count)] = xin[order(m)].astype(F32) + added
    early_rows = 2 * row_count // (4 * BLOCK) * (4 * BLOCK)
    sweep(early_rows // BLOCK, first_norm, ())
    load_qkv.wait()
    project(0, early_rows)

    for copy in into_x[0][1:]:
        copy.wait_recv()
    sent(into_x)
    for j in range(strips):
        outgoing[j] = cotangent[:, j, :]
    launch(into_c)
    for m in range(2, strips):
        hidden[pl.ds(m * row_count, row_count)] = xin[order(m)].astype(F32) + added
    sweep(blocks, first_norm, (), early_rows // BLOCK)
    project(early_rows, rows - early_rows)

    @pl.loop(0, width // 128)
    def _(pair):
        attend_pair(pair, seen(), proj, mixed, lse_all)

    arrive(into_c)
    for j in range(strips):
        gn[pl.ds(j * row_count, row_count)] = cin[order(j)].astype(F32)
    load_out.wait()
    att[...] = hidden[...] + dot(mixed[...], wout[...], 1, 0) + row(out_bias)
    zero8 = jnp.zeros((8, width), F32)

    def second_norm(b):
        at = block_rows(b)
        block = att[at]
        normed, _ = standardize(block)
        upstream = gn[at]
        stores = [
            (n2, at, (normed * row(gain_two) + row(bias_two)).astype(BF)),
            (res, at, block + row(down_bias)),
            (cot, at, upstream.astype(BF)),
            (gn, at, jnp.zeros((BLOCK, width), F32)),
        ]
        return stores, (fold(upstream),)

    early[pl.ds(3, 1)] = column_sum(sweep(blocks, second_norm, (zero8,))[0])

    @pl.loop(0, ff_blocks)
    def _(block):
        slot = block % 2
        for copy in load_ff(block):
            copy.wait()

        @pl.when(block + 1 < ff_blocks)
        def _():
            for copy in load_ff(block + 1):
                copy.start()

        up = wup[slot]
        down = wdown[slot]
        upper = dot(n2[...], up, 1, 0) + ubias[pl.ds(block, 1)]
        grad_active = dot(cot[...], down, 1, 1)
        share = 0.5 * (1.0 + erf(upper * 0.7071067811865476))
        act[...] = (upper * share).astype(BF)
        slope = share + upper * jnp.exp(-0.5 * upper * upper) * 0.3989422804014327
        grad_upper = (grad_active * slope).astype(BF)
        gblk[...] = grad_upper
        res[...] += dot(act[...], down, 1, 0)
        gn[...] += dot(grad_upper, up, 1, 1)
        early[pl.ds(4 + block, 1)] = column_sum(grad_upper.astype(F32))
        red.step(PLAN["ffn"][0], block)
        product[...] = dot(n2[...], gblk[...], 0, 0).astype(BF)
        for half in range(2):
            c = 2 * block + half
            red.free(c, False)
            red.place(c, half, product)
            red.start(c, False)
        red.step(PLAN["ffn"][1], block)
        product[...] = dot(act[...], cot[...], 0, 0).astype(BF)
        for half in range(2):
            c = OWN + 2 * block + half
            red.free(c, True)
            red.place_down(c, half, product)
            red.start(c, True)
        red.step(PLAN["ffn"][2], block)

    sent(into_c)
    for j in range(strips):
        outgoing[order(j)] = res[pl.ds(j * row_count, row_count)].astype(BF)
    from_out = exchange(2, outgoing, layer_out)
    launch(from_out)

    def second_back(b):
        at = block_rows(b)
        normed, inverse = standardize(att[at])
        upstream = gn[at]
        scaled = upstream * row(gain_two)
        back = inverse * (scaled - mean(scaled) - normed * mean(scaled * normed))
        grad = cot[at].astype(F32) + back
        rounded = grad.astype(BF)
        sums = (fold(upstream * normed), fold(upstream), fold(rounded.astype(F32)))
        return [(gn, at, grad), (branch, at, rounded)], sums

    totals = sweep(blocks, second_back, (zero8, zero8, zero8))
    early[pl.ds(0, 1)] = column_sum(totals[0])
    early[pl.ds(1, 1)] = column_sum(totals[1])
    early[pl.ds(2, 1)] = column_sum(totals[2])
    share_early = share(0, early, early_in)
    share_early[0](0)
    red.step(PLAN["after"][:1])
    gmixed[...] = dot(branch[...], wout[...], 1, 1).astype(BF)
    red.step(PLAN["after"][1:2])
    product[...] = dot(mixed[...], branch[...], 0, 0).astype(BF)
    for half in range(2):
        c = 8 + half
        red.free(c, False)
        red.place(c, half, product)
        red.start(c, False)
    red.step(PLAN["after"][2:])

    res[...] = jnp.zeros_like(res)

    @pl.loop(0, 3)
    def _(i):
        @pl.loop(0, 2)
        def _(h):
            pair = 2 * i + h
            grads = attend_pair_back(pair, seen(), proj, gmixed, lse_all)
            for part in range(3):
                gblk[:, pl.ds(pl.multiple_of(h * WIDE + part * 128, 128), 128)] = grads[part]
            lanes = pl.ds(pl.multiple_of(pair * 128, 128), 128)
            late[pl.ds(2, 1), lanes] = column_sum(grads[0].astype(F32))
            late[pl.ds(3, 1), lanes] = column_sum(grads[2].astype(F32))
            red.step(PLAN["pair"], pair)

        product[...] = dot(n1[...], gblk[...], 0, 0).astype(BF)
        for half in range(2):
            c = 10 + 2 * i + half
            red.free(c, False)
            red.place(c, half, product)
            red.start(c, False)
        red.step(PLAN["grad"][0], i)
        weights = jnp.concatenate(
            [
                wqkv[:, pl.ds(pl.multiple_of(part * width + (2 * i + h) * 128, 128), 128)]
                for h in range(2)
                for part in range(3)
            ],
            axis=1,
        )
        res[...] += dot(gblk[...], weights, 1, 1)
        red.step(PLAN["grad"][1], i)
        for turn in range(3):

            @pl.when(i == turn)
            def _():
                share_early[1](turn)

    def first_back(b):
        at = block_rows(b)
        normed, inverse = standardize(hidden[at])
        upstream = res[at]
        scaled = upstream * row(gain_one)
        back = inverse * (scaled - mean(scaled) - normed * mean(scaled * normed))
        grad = gn[at] + back
        return [(res, at, grad)], (fold(upstream * normed), fold(upstream), fold(grad))

    totals = sweep(blocks, first_back, (zero8, zero8, zero8))
    red.step(PLAN["last"][:1])
    late[pl.ds(0, 1)] = column_sum(totals[0])
    late[pl.ds(1, 1)] = column_sum(totals[1])
    strip_sum = column_sum(totals[2])
    for group in range(table.shape[0]):
        late[pl.ds(4 + group, 1)] = jnp.where(own_script == group, strip_sum, 0.0)
    share_late = share(1, late, late_in)
    share_late[0](0)
    for j in range(strips):
        xin[order(j)] = res[pl.ds(j * row_count, row_count)].astype(BF)
    from_grad = exchange(3, xin, grad_patches)
    red.step(PLAN["last"][1:])
    tail = PLAN["tail"]
    turns = [len(tail) * (turn + 1) // 4 for turn in range(3)]
    waiting = True
    for index in range(len(tail)):
        red.step(tail[index : index + 1])
        if waiting and tail[index][2 * STAGES + 1] == OWN:
            launch(from_grad)
            waiting = False
        for turn in range(3):
            if turns[turn] == index:
                share_late[1](turn)

    owner = s * strips + q
    spread = lax.broadcasted_iota(jnp.int32, (width, 128), 0)
    lane = lax.broadcasted_iota(jnp.int32, (width, 128), 1)
    few = jnp.where((spread == PART * owner + lane) & (lane < PART), 1.0, 0.0)
    many = jnp.where((spread == 4 * PART * (owner % 8) + lane) & (lane < 4 * PART), 1.0, 0.0)
    exact = lambda left, right: lax.dot_general(
        left, right, (((1,), (0,)), ((), ())), precision=lax.Precision.HIGHEST,
        preferred_element_type=F32,
    )
    lines = lax.broadcasted_iota(jnp.int32, (8, width), 0)
    chosen = jnp.where(lines == 4 + owner // 8, early[...], 0.0)
    small[pl.ds(0, 8)] = exact(early[...], few)
    small[pl.ds(8, 8)] = exact(late[...], few)
    small[pl.ds(16, 8)] = exact(chosen, many)

    red.finish()
    for moves in (from_out, from_grad):
        arrive(moves)
        sent(moves)


def run_layer(*arrays):
    patches = arrays[12]
    row_count, strips, width = patches.shape
    rows = -(-strips * row_count // BLOCK) * BLOCK
    vmem = pl.BlockSpec(memory_space=pltpu.VMEM)
    smem = pl.BlockSpec(memory_space=pltpu.SMEM)
    hbm = pl.BlockSpec(memory_space=pl.ANY)
    packed = lambda *shape: pltpu.VMEM(shape, BF)
    wide = lambda *shape: pltpu.VMEM(shape, F32)
    return pl.pallas_call(
        layer_kernel,
        out_shape=[
            jax.ShapeDtypeStruct((strips, row_count, width), BF),
            jax.ShapeDtypeStruct((strips, row_count, width), BF),
            jax.ShapeDtypeStruct((OWN, PART, WIDE), F32),
            jax.ShapeDtypeStruct((2, 4 * PART, WIDE), F32),
            jax.ShapeDtypeStruct((24, 128), F32),
        ],
        in_specs=[smem] * 2 + [vmem] * 12 + [hbm] * 4,
        out_specs=[hbm, hbm, vmem, vmem, vmem],
        scratch_shapes=[
            packed(strips, row_count, width),
            packed(strips, row_count, width),
            packed(strips, row_count, width),
            wide(rows, width),
            packed(rows, width),
            packed(rows, 3 * width),
            packed(rows, width),
            wide(rows, 128),
            wide(rows, width),
            packed(rows, width),
            packed(rows, width),
            wide(rows, width),
            wide(rows, width),
            packed(rows, width),
            packed(rows, width),
            packed(rows, width),
            packed(rows, width),
            packed(width, width),
            wide(8, width),
            wide(8, width),
            wide(8, width),
            wide(8, width),
            packed(width, 3 * width),
            packed(width, width),
            packed(2, width, width),
            packed(2, width, width),
            packed(2 * SLOTS, 2, 384, WIDE),
            packed(CHUNKS, 384, WIDE),
            packed(CHUNKS, 192, WIDE),
            packed(CHUNKS, 96, WIDE),
            packed(OWN, 48, WIDE),
            packed(OWN, 2, 24, WIDE),
            packed(OWN, 24, WIDE),
            packed(CHUNKS - OWN, 96, WIDE),
            packed(CHUNKS - OWN, 96, WIDE),
        ]
        + [wide(7, 8, width)] * 2
        + [
            pltpu.SemaphoreType.DMA((STAGES, CHUNKS)),
            pltpu.SemaphoreType.DMA((STAGES, CHUNKS)),
            pltpu.SemaphoreType.DMA((2, 7)),
            pltpu.SemaphoreType.DMA((2, 7)),
            pltpu.SemaphoreType.DMA((4, strips)),
            pltpu.SemaphoreType.DMA((4, strips)),
            pltpu.SemaphoreType.DMA((2,)),
            pltpu.SemaphoreType.DMA((2, 2)),
            pltpu.SemaphoreType.DMA((4,)),
        ],
        compiler_params=pltpu.CompilerParams(
            collective_id=0, has_side_effects=True, vmem_limit_bytes=67043328
        ),
    )(*arrays)


def finish_kernel(
    layer_in, grad_in, reduced, reduced_down, small,
    layer_out, grad_patches, table, gain_one, bias_one, qkv, query_bias, value_bias, out_weight,
    out_bias, gain_two, bias_two, up_weight, up_bias, down_weight, down_bias,
):
    for j in range(layer_in.shape[0]):
        layer_out[:, j, :] = layer_in[j]
        grad_patches[:, j, :] = grad_in[j]
    names = {
        0: gain_two, 1: bias_two, 2: out_bias, 3: down_bias,
        8: gain_one, 9: bias_one, 10: query_bias, 11: value_bias,
    }
    for index, ref in names.items():
        ref[...] = small[pl.ds(index, 1), pl.ds(0, PART)].reshape(PART)
    up_bias[...] = column_sum(small[pl.ds(16, 8), pl.ds(0, 4 * PART)]).reshape(4 * PART)
    table[...] = small[pl.ds(12, 4), pl.ds(0, PART)]
    for c in range(8):
        up_weight[:, pl.ds(c * WIDE, WIDE)] = reduced[c]
    for c in range(2):
        out_weight[:, pl.ds(c * WIDE, WIDE)] = reduced[8 + c]
    for half in range(2):
        down_weight[:, pl.ds(half * WIDE, WIDE)] = reduced_down[half]
    width = qkv.shape[1] // 3
    for pair in range(6):
        for part in range(3):
            qkv[:, pl.ds(part * width + pair * 128, 128)] = reduced[
                10 + pair, :, pl.ds(part * 128, 128)
            ]


def local(
    patches,
    lengths,
    script,
    script_table,
    gain_one,
    bias_one,
    qkv_weight,
    query_bias,
    value_bias,
    out_weight,
    out_bias,
    gain_two,
    bias_two,
    up_weight,
    up_bias,
    down_weight,
    down_bias,
    cotangent,
):
    strips, row_count, width = patches.shape
    groups = script_table.shape[0]
    results = run_layer(
        lengths, script, script_table, gain_one, bias_one, query_bias, value_bias, out_bias,
        gain_two, bias_two, up_bias, down_bias, patches.transpose(1, 0, 2),
        cotangent.transpose(1, 0, 2), qkv_weight,
        out_weight, up_weight, down_weight,
    )
    vector = jax.ShapeDtypeStruct((PART,), F32)
    turned = jax.ShapeDtypeStruct((row_count, strips, width), BF)
    outputs = pl.pallas_call(
        finish_kernel,
        out_shape=[
            turned,
            turned,
            jax.ShapeDtypeStruct((groups, PART), F32),
            vector,
            vector,
            jax.ShapeDtypeStruct((PART, 3 * width), F32),
            vector,
            vector,
            jax.ShapeDtypeStruct((PART, width), F32),
            vector,
            vector,
            vector,
            jax.ShapeDtypeStruct((PART, up_weight.shape[1]), F32),
            jax.ShapeDtypeStruct((4 * PART,), F32),
            jax.ShapeDtypeStruct((4 * PART, width), F32),
            vector,
        ],
    )(*results)
    return (
        outputs[0].transpose(1, 0, 2),
        outputs[1].transpose(1, 0, 2),
        outputs[2].T,
        *outputs[3:],
    )


def solution(mesh):
    placed = (
        P("strip", "seq", None),
        P("strip"),
        P("strip"),
        P(),
        P(),
        P(),
        P(),
        P(),
        P(),
        P(),
        P(),
        P(),
        P(),
        P(),
        P(),
        P(),
        P(),
        P("strip", "seq", None),
    )
    chosen = local if fits(mesh) else local_general
    return jax.shard_map(
        chosen,
        mesh=mesh,
        in_specs=placed,
        out_specs=(
            P("strip", "seq", None),
            P("strip", "seq", None),
            P(("strip", "seq"), None),
            P(("strip", "seq")),
            P(("strip", "seq")),
            P(("strip", "seq"), None),
            P(("strip", "seq")),
            P(("strip", "seq")),
            P(("strip", "seq"), None),
            P(("strip", "seq")),
            P(("strip", "seq")),
            P(("strip", "seq")),
            P(("strip", "seq"), None),
            P(("strip", "seq")),
            P(("strip", "seq"), None),
            P(("strip", "seq")),
        ),
        check_vma=False,
    )
```
